128 devices in a mesh: ia: 16 (over y, x), ja: 4 (over z_lo, core), col: 2 (over z_hi).
Axes of the slice: x: 4, y: 4, z: 4 (z_hi: 2, z_lo: 2; z = z_hi * 2 + z_lo), core: 2. Of those that a mesh axis runs over, the one named last changes fastest.
Arguments:
- pair_rep: bfloat16 [512, 512, 128], P('ia', 'ja'), may hold values from -6 to 6
- norm_gain: float32 [128], replicated, may hold values from 0.1 to 1.9
- weights: bfloat16 [4, 128, 128], P(None, None, 'col'), may hold values from -0.5 to 0.5
- residue_mask: int32 [512], replicated, may hold values 0 or 1
- product_grad: bfloat16 [512, 128, 512], P('ia', 'col', 'ja'), may hold values from -1 to 1
Outputs:
- pair_grad: bfloat16 [512, 512, 128], P('ia', 'ja')
- weight_grads: float32 [4, 128, 128], P(None, None, 'col')
The draws below stay inside these ranges and needn't reach their ends.
All inputs are finite; a program needn't handle non-finite values.
Results may differ from the reference program's by a relative error of at most 0.0067.
Values may be sent and summed in bfloat16 or wider, within the bound.
No kernel may reach another device: no remote copies, remote signals or barrier semaphores. Data moves between devices by JAX's collectives and lax.ppermute only.
A program may use at most 128 MiB of HBM per device.

```python
import jax
import jax.numpy as jnp
from jax import lax

C = 128
HID = 128
N = 512


def draw_product_grad(key, part):
    gaussian = jax.random.normal(jax.random.fold_in(key, 11), (N, HID, N), jnp.float32)
    drawn = 0.0625 * gaussian
    return jnp.clip(drawn, -1.0, 1.0).astype(jnp.bfloat16)


def set_ends(result, own_key, least, largest):
    longest = result.shape.index(max(result.shape))
    spots = []
    for shift in (0, 1):
        where = [jax.random.randint(jax.random.fold_in(own_key, axis), (), 0, length) for axis, length in enumerate(result.shape)]
        where[longest] = (where[longest] + shift) % result.shape[longest]
        spots.append(tuple(where))
    return result.at[spots[0]].set(least).at[spots[1]].set(largest)


def levels(rng, extent, shards, least, largest):
    level, own = 1.0, jax.random.fold_in(rng, 6)
    for dim, blocks in shards:
        steps = jnp.exp(jax.random.uniform(jax.random.fold_in(own, dim), (blocks,), jnp.float32, least / len(shards), largest / len(shards)))
        level = level * jnp.repeat(steps, extent[dim] // blocks).reshape([-1 if axis == dim else 1 for axis in range(len(extent))])
    return level


def noise(stream_key, dims, width, reach, shards=(), held_as=jnp.bfloat16):
    level = levels(stream_key, dims, shards, -0.22, 0.18) if shards else 1.0
    entries = jax.random.normal(stream_key, dims, jnp.float32) * width * level
    return jnp.minimum(jnp.maximum(entries, -reach), reach).astype(held_as)


def setup_inputs(seed: int = 0) -> dict:
    seeds = jax.random.split(jax.random.key(seed), 6)
    pair_rep = noise(seeds[0], (N, N, C), 1.0, 6.0, ((0, 16), (1, 4)))
    norm_gain = jnp.clip(1.0 + 0.18 * jax.random.normal(seeds[1], (C,), jnp.float32), 0.1, 1.9)
    weights = noise(seeds[2], (4, C, HID), C ** -0.5, 0.5, ((2, 2),))
    residue_mask = set_ends((jax.random.randint(seeds[3], (N,), 0, 8) < 7).astype(jnp.int32), jax.random.fold_in(seeds[3], 1), 0, 1)
    product_grad = draw_product_grad(jax.random.fold_in(seeds[5], 71), 0)
    return {"pair_rep": pair_rep, "norm_gain": norm_gain, "weights": weights, "residue_mask": residue_mask, "product_grad": product_grad}


CLIP_LIMIT = 64.0

def gate_terms(incoming, linear, gate_pre, pair_valid):
    sigmoid_gate = jax.nn.sigmoid(gate_pre)
    through = incoming * pair_valid
    return (through * sigmoid_gate, through * linear * sigmoid_gate * (1.0 - sigmoid_gate))

def reference(pair_rep, norm_gain, weights, residue_mask, product_grad):
    floats = pair_rep.astype(jnp.float32)
    centred = floats - lax.optimization_barrier(jnp.mean(floats, axis=-1, keepdims=True))
    inv_std = lax.rsqrt(lax.optimization_barrier(jnp.mean(centred * centred, axis=-1, keepdims=True)) + 1e-05)
    unit_rows = centred * inv_std
    normed = (unit_rows * norm_gain).astype(jnp.bfloat16)
    validity = residue_mask.astype(jnp.float32)
    pair_valid = validity[:, None, None] * validity[None, None, :]
    normed_wide = normed.astype(jnp.float32)
    weights_wide = weights.astype(jnp.float32)
    projected = [jnp.einsum('ikd,dc->ick', normed_wide, weights_wide[which]) for which in range(4)]
    left_side = (pair_valid * jax.nn.sigmoid(projected[1]) * projected[0]).astype(jnp.bfloat16)
    right_side = (pair_valid * jax.nn.sigmoid(projected[3]) * projected[2]).astype(jnp.bfloat16)
    grad_wide = product_grad.astype(jnp.float32)
    grad_left = jnp.einsum('icj,jck->ick', grad_wide, right_side.astype(jnp.float32))
    grad_right = jnp.einsum('icj,ick->jck', grad_wide, left_side.astype(jnp.float32))
    lin_a, gate_a = gate_terms(grad_left, projected[0], projected[1], pair_valid)
    lin_b, gate_b = gate_terms(grad_right, projected[2], projected[3], pair_valid)
    raw_list = []
    normed_grad = jnp.zeros(floats.shape, jnp.float32)
    for which, term in enumerate((lin_a, gate_a, lin_b, gate_b)):
        rounded = lax.optimization_barrier(term.astype(jnp.bfloat16)).astype(jnp.float32)
        raw_list.append(jnp.einsum('ikd,ick->dc', normed_wide, rounded))
        normed_grad = normed_grad + jnp.einsum('ick,dc->ikd', rounded, weights_wide[which])
    scaled = normed_grad * norm_gain
    pair_grad = inv_std * (scaled - lax.optimization_barrier(jnp.mean(scaled, axis=-1, keepdims=True)) - unit_rows * lax.optimization_barrier(jnp.mean(scaled * unit_rows, axis=-1, keepdims=True)))
    raw = jnp.stack(raw_list)
    squares = jnp.sum(raw * raw)
    factor = jnp.minimum(1.0, CLIP_LIMIT * lax.rsqrt(squares + 1e-06))
    return (pair_grad.astype(jnp.bfloat16), raw * factor)
```

```python
import functools

import jax
import jax.numpy as jnp
from jax import lax
from jax.experimental import pallas as pl
from jax.experimental.pallas import tpu as pltpu
from jax.sharding import PartitionSpec as P

CLIP_LIMIT = 64.0
BF, F32 = jnp.bfloat16, jnp.float32


def normalised(x, gain=None):
    mean = jnp.mean(x, axis=-1, keepdims=True)
    centred = x - mean
    inv_std = lax.rsqrt(jnp.mean(centred * centred, axis=-1, keepdims=True) + 1e-05)
    return centred * inv_std, inv_std


def channels_first_kernel(x_ref, out_ref, flat):
    rows, chans, width = x_ref.shape
    flat[...] = x_ref[...].reshape(rows * chans, width).astype(F32)
    for c in range(chans):
        out_ref[c] = flat[pl.ds(c, rows, stride=chans), :].astype(BF)


def channels_first(x):
    rows, chans, width = x.shape
    return pl.pallas_call(
        channels_first_kernel,
        out_shape=jax.ShapeDtypeStruct((chans, rows, width), BF),
        scratch_shapes=[pltpu.VMEM((rows * chans, width), F32)],
        cost_estimate=pl.CostEstimate(flops=10**6, bytes_accessed=2 * x.size * 2, transcendentals=0),
        name="channels_first",
    )(x)


def project_kernel(x_ref, gain_ref, w_ref, valid_ref, sides_ref, factors_ref, normed_ref, flat):
    rows = x_ref.shape[0]
    groups, _, per, _, _ = sides_ref.shape
    half = groups * per
    gain = gain_ref[...]
    w = w_ref[...]

    def row(i, carry):
        unit, _ = normalised(x_ref[i].astype(F32))
        normed = (unit * gain).astype(BF)
        normed_ref[i] = normed
        proj = lax.dot_general(w, normed, (((1,), (1,)), ((), ())), preferred_element_type=F32)
        valid = valid_ref[pl.ds(i, 1), :]
        for side in range(2):
            at = 2 * side * half
            linear = proj[at : at + half]
            gate = jax.nn.sigmoid(proj[at + half : at + 2 * half])
            first = valid * gate
            both = first * linear
            flat[pl.ds(pl.multiple_of(i * 2 * half + side * half, half), half), :] = both
            factors_ref[i, at : at + half, :] = first
            factors_ref[i, at + half : at + 2 * half, :] = both * (1.0 - gate)
        return carry

    lax.fori_loop(0, rows, row, 0, unroll=2)
    for g in range(groups):
        for side in range(2):
            for c in range(per):
                first = side * half + g * per + c
                sides_ref[g, side, c] = flat[pl.ds(first, rows, stride=2 * half), :].astype(BF)


def project(x, gain, w, valid, groups, step):
    rows, cols, depth = x.shape
    half = w.shape[0] // 4
    per = half // groups
    return pl.pallas_call(
        project_kernel,
        grid=(rows // step,),
        in_specs=[
            pl.BlockSpec((step, cols, depth), lambda r: (r, 0, 0)),
            pl.BlockSpec((1, depth), lambda r: (0, 0)),
            pl.BlockSpec(w.shape, lambda r: (0, 0)),
            pl.BlockSpec((step, cols), lambda r: (r, 0)),
        ],
        out_specs=[
            pl.BlockSpec((groups, 2, per, step, cols), lambda r: (0, 0, 0, r, 0)),
            pl.BlockSpec((step, 4 * half, cols), lambda r: (r, 0, 0)),
            pl.BlockSpec((step, cols, depth), lambda r: (r, 0, 0)),
        ],
        out_shape=[
            jax.ShapeDtypeStruct((groups, 2, per, rows, cols), BF),
            jax.ShapeDtypeStruct((rows, 4 * half, cols), F32),
            jax.ShapeDtypeStruct((rows, cols, depth), BF),
        ],
        scratch_shapes=[pltpu.VMEM((step * 2 * half, cols), F32)],
        cost_estimate=pl.CostEstimate(flops=6 * 10**9, bytes_accessed=7 * 2**20, transcendentals=10**6),
        name="project",
    )(x, gain, w, valid)


def triangle_kernel(at_ref, sides_ref, *refs):
    *grads, out_ref = refs
    groups, _, _, rows, cols = sides_ref.shape
    share = groups // len(grads)
    left = sides_ref[:, 0, 0].reshape(groups * rows, cols)
    total = None
    for t, grad_ref in enumerate(grads):
        first = at_ref[t] * share
        grad = grad_ref[:, 0].reshape(groups * rows, cols)
        right = sides_ref[pl.ds(first, share), 1, 0].reshape(share * rows, cols)
        part = jnp.dot(grad, right, preferred_element_type=F32)
        total = part if total is None else total + part
        back = lax.dot_general(grad, left, (((0,), (0,)), ((), ())), preferred_element_type=F32)
        out_ref[pl.ds(first, share), 1, 0] = back.astype(BF).reshape(share, rows, cols)
    out_ref[:, 0, 0] = total.astype(BF).reshape(groups, rows, cols)


def triangle(at, sides, grads):
    groups, _, per, rows, cols = sides.shape
    side_spec = pl.BlockSpec((groups, 2, 1, rows, cols), lambda c, at: (0, 0, c, 0, 0))
    grad_spec = pl.BlockSpec((groups, 1, rows, cols), lambda c, at: (0, c, 0, 0))
    return pl.pallas_call(
        triangle_kernel,
        grid_spec=pltpu.PrefetchScalarGridSpec(
            num_scalar_prefetch=1,
            grid=(per,),
            in_specs=[side_spec] + [grad_spec] * len(grads),
            out_specs=side_spec,
        ),
        out_shape=jax.ShapeDtypeStruct(sides.shape, BF),
        cost_estimate=pl.CostEstimate(flops=4 * 10**9, bytes_accessed=5 * 2**20, transcendentals=0),
        name="triangle",
    )(at, sides, *grads)


def gate_kernel(in_ref, factors_ref, normed_ref, w_ref, out_ref, raw_ref, flat):
    groups, _, per, rows, _ = in_ref.shape
    half = groups * per
    for g in range(groups):
        for side in range(2):
            for c in range(per):
                first = (side * half + g * per + c) * rows
                flat[first : first + rows, :] = in_ref[g, side, c].astype(F32)

    @pl.when(pl.program_id(0) == 0)
    def _():
        raw_ref[...] = jnp.zeros_like(raw_ref)

    w = w_ref[...]

    def pair(i2, carry):
        made = []
        for e in range(2):
            i = i2 * 2 + e
            parts = []
            for side in range(2):
                incoming = flat[pl.ds(side * half * rows + i, half, stride=rows), :]
                at = 2 * side * half
                parts.append((incoming * factors_ref[i, at : at + half, :]).astype(BF))
                parts.append((incoming * factors_ref[i, at + half : at + 2 * half, :]).astype(BF))
            grads = jnp.concatenate(parts, axis=0)
            made.append(grads)
            back = lax.dot_general(grads, w, (((0,), (0,)), ((), ())), preferred_element_type=F32)
            out_ref[i] = back.astype(BF)
        both = jnp.concatenate(made, axis=1)
        cols, depth = normed_ref.shape[1:]
        normed = normed_ref[pl.ds(i2 * 2, 2)].reshape(2 * cols, depth)
        raw_ref[...] += jnp.dot(both, normed, preferred_element_type=F32)
        return carry

    lax.fori_loop(0, rows // 2, pair, 0)


def gate(incoming, factors, normed, w, step):
    groups, _, per, rows, cols = incoming.shape
    depth = normed.shape[-1]
    return pl.pallas_call(
        gate_kernel,
        grid=(rows // step,),
        in_specs=[
            pl.BlockSpec((groups, 2, per, step, cols), lambda r: (0, 0, 0, r, 0)),
            pl.BlockSpec((step,) + factors.shape[1:], lambda r: (r, 0, 0)),
            pl.BlockSpec((step, cols, depth), lambda r: (r, 0, 0)),
            pl.BlockSpec(w.shape, lambda r: (0, 0)),
        ],
        out_specs=[
            pl.BlockSpec((step, cols, depth), lambda r: (r, 0, 0)),
            pl.BlockSpec(w.shape, lambda r: (0, 0)),
        ],
        out_shape=[
            jax.ShapeDtypeStruct((rows, cols, depth), BF),
            jax.ShapeDtypeStruct(w.shape, F32),
        ],
        scratch_shapes=[pltpu.VMEM((2 * groups * per * step, cols), F32)],
        cost_estimate=pl.CostEstimate(flops=6 * 10**9, bytes_accessed=8 * 2**20, transcendentals=0),
        name="gate",
    )(incoming, factors, normed, w)


def finish_kernel(x_ref, gain_ref, own_ref, other_ref, out_ref):
    unit, inv_std = normalised(x_ref[...].astype(F32))
    scaled = (own_ref[...].astype(F32) + other_ref[...].astype(F32)) * gain_ref[...]
    mean = jnp.mean(scaled, axis=-1, keepdims=True)
    along = jnp.mean(scaled * unit, axis=-1, keepdims=True)
    out_ref[...] = (inv_std * (scaled - mean - unit * along)).astype(BF)


def finish(x, gain, own, other, step):
    rows, cols, depth = x.shape
    spec = pl.BlockSpec((step, cols, depth), lambda r: (r, 0, 0))
    return pl.pallas_call(
        finish_kernel,
        grid=(rows // step,),
        in_specs=[spec, pl.BlockSpec((1, 1, depth), lambda r: (0, 0, 0)), spec, spec],
        out_specs=spec,
        out_shape=jax.ShapeDtypeStruct(x.shape, BF),
        cost_estimate=pl.CostEstimate(flops=10**7, bytes_accessed=4 * 2**20, transcendentals=0),
        name="finish",
    )(x, gain.reshape(1, 1, depth), own, other)


def swapped(x, axis, bit):
    size = lax.axis_size(axis)
    return lax.ppermute(x, axis, [(i, i ^ bit) for i in range(size)])


def on_device(pair_rep, norm_gain, weights, residue_mask, product_grad):
    rows, cols, depth = pair_rep.shape
    chans = product_grad.shape[1]
    groups = lax.axis_size("ia")
    per = chans // groups
    here = lax.axis_index("ja")
    validity = residue_mask.astype(F32)
    row_valid = lax.dynamic_slice_in_dim(validity, lax.axis_index("ia") * rows, rows)
    col_valid = lax.dynamic_slice_in_dim(validity, here * cols, cols)
    pair_valid = row_valid[:, None] * col_valid[None, :]
    w = jnp.swapaxes(weights, 1, 2).reshape(4 * chans, depth)

    grads = channels_first(product_grad).reshape(groups, per, rows, cols)
    grads = lax.all_to_all(grads, "ia", 0, 0, tiled=True)
    far = swapped(grads, "ja", 2)
    sides, factors, normed = project(pair_rep, norm_gain[None], w, pair_valid, groups, 16)
    sides = lax.all_to_all(sides, "ia", 0, 0, tiled=True)
    near = swapped(grads, "ja", 1)
    farther = swapped(far, "ja", 1)
    at = jnp.stack([here, here ^ 1, here ^ 2, here ^ 3]).astype(jnp.int32)
    products = triangle(at, sides, (grads, near, far, farther))
    products = lax.all_to_all(products, "ia", 0, 0, tiled=True)
    own, raw = gate(products, factors, normed, w, 16)
    other = swapped(own, "col", 1)

    peers = ("ia", "ja")
    count = lax.axis_size(peers)
    pieces = lax.all_to_all(raw.reshape(count, -1, depth), peers, 0, 0, tiled=True)
    piece = jnp.sum(pieces, axis=0)
    whole = lax.all_to_all(jnp.broadcast_to(piece[None], pieces.shape), peers, 0, 0, tiled=True)
    whole = whole.reshape(4, chans, depth)
    squares = jnp.sum(whole * whole).reshape(1, 1)
    squares = squares + swapped(squares, "col", 1)
    factor = jnp.minimum(1.0, CLIP_LIMIT * lax.rsqrt(squares[0, 0] + 1e-06))
    weight_grads = jnp.swapaxes(whole, 1, 2) * factor
    pair_grad = finish(pair_rep, norm_gain, own, other, 8)
    return (pair_grad, weight_grads)


def solution(mesh):
    placed = (P("ia", "ja", None), P(), P(None, None, "col"), P(), P("ia", "col", "ja"))
    return jax.shard_map(
        on_device,
        mesh=mesh,
        in_specs=placed,
        out_specs=(P("ia", "ja", None), P(None, None, "col")),
        check_vma=False,
    )
```

```python
import jax
import jax.numpy as jnp
from jax import lax
from jax.experimental import pallas as pl
from jax.experimental.pallas import tpu as pltpu
from jax.sharding import PartitionSpec as P


CLIP_LIMIT = 64.0
BF, F32 = jnp.bfloat16, jnp.float32


def normalised(x):
    mean = jnp.mean(x, axis=-1, keepdims=True)
    centred = x - mean
    inv_std = lax.rsqrt(jnp.mean(centred * centred, axis=-1, keepdims=True) + 1e-05)
    return centred * inv_std, inv_std


def channels_first_kernel(x_ref, out_ref, flat):
    rows, chans, width = x_ref.shape
    flat[...] = x_ref[...].reshape(rows * chans, width).astype(F32)
    for c in range(chans):
        out_ref[c] = flat[pl.ds(c, rows, stride=chans), :].astype(BF)


def channels_first(x):
    rows, chans, width = x.shape
    return pl.pallas_call(
        channels_first_kernel,
        out_shape=jax.ShapeDtypeStruct((chans, rows, width), BF),
        scratch_shapes=[pltpu.VMEM((rows * chans, width), F32)],
        cost_estimate=pl.CostEstimate(flops=10**6, bytes_accessed=2 * x.size * 2, transcendentals=0),
        name="channels_first",
    )(x)


def project_kernel(x_ref, gain_ref, w_ref, valid_ref, sides_ref, factors_ref, normed_ref, flat):
    rows = x_ref.shape[0]
    groups, _, per, _, _ = sides_ref.shape
    half = groups * per
    gain = gain_ref[...]
    w = w_ref[...]

    def row(i, carry):
        unit, _ = normalised(x_ref[i].astype(F32))
        normed = (unit * gain).astype(BF)
        normed_ref[i] = normed
        proj = lax.dot_general(w, normed, (((1,), (1,)), ((), ())), preferred_element_type=F32)
        valid = valid_ref[pl.ds(i, 1), :]
        for side in range(2):
            at = 2 * side * half
            linear = proj[at : at + half]
            gate = jax.nn.sigmoid(proj[at + half : at + 2 * half])
            first = valid * gate
            both = first * linear
            flat[pl.ds(pl.multiple_of(i * 2 * half + side * half, half), half), :] = both
            factors_ref[i, at : at + half, :] = first
            factors_ref[i, at + half : at + 2 * half, :] = both * (1.0 - gate)
        return carry

    lax.fori_loop(0, rows, row, 0, unroll=2)
    for g in range(groups):
        for side in range(2):
            for c in range(per):
                first = side * half + g * per + c
                sides_ref[g, side, c] = flat[pl.ds(first, rows, stride=2 * half), :].astype(BF)


def project(x, gain, w, valid, groups, step):
    rows, cols, depth = x.shape
    half = w.shape[0] // 4
    per = half // groups
    return pl.pallas_call(
        project_kernel,
        grid=(rows // step,),
        in_specs=[
            pl.BlockSpec((step, cols, depth), lambda r: (r, 0, 0)),
            pl.BlockSpec((1, depth), lambda r: (0, 0)),
            pl.BlockSpec(w.shape, lambda r: (0, 0)),
            pl.BlockSpec((step, cols), lambda r: (r, 0)),
        ],
        out_specs=[
            pl.BlockSpec((groups, 2, per, step, cols), lambda r: (0, 0, 0, r, 0)),
            pl.BlockSpec((step, 4 * half, cols), lambda r: (r, 0, 0)),
            pl.BlockSpec((step, cols, depth), lambda r: (r, 0, 0)),
        ],
        out_shape=[
            jax.ShapeDtypeStruct((groups, 2, per, rows, cols), BF),
            jax.ShapeDtypeStruct((rows, 4 * half, cols), F32),
            jax.ShapeDtypeStruct((rows, cols, depth), BF),
        ],
        scratch_shapes=[pltpu.VMEM((step * 2 * half, cols), F32)],
        cost_estimate=pl.CostEstimate(flops=6 * 10**9, bytes_accessed=7 * 2**20, transcendentals=10**6),
        name="project",
    )(x, gain, w, valid)


def triangle_kernel(at_ref, sides_ref, *refs):
    *grads, out_ref = refs
    groups, _, _, rows, cols = sides_ref.shape
    share = groups // len(grads)
    left = sides_ref[:, 0, 0].reshape(groups * rows, cols)
    total = None
    for t, grad_ref in enumerate(grads):
        first = at_ref[t] * share
        grad = grad_ref[:, 0].reshape(groups * rows, cols)
        right = sides_ref[pl.ds(first, share), 1, 0].reshape(share * rows, cols)
        part = jnp.dot(grad, right, preferred_element_type=F32)
        total = part if total is None else total + part
        back = lax.dot_general(grad, left, (((0,), (0,)), ((), ())), preferred_element_type=F32)
        out_ref[pl.ds(first, share), 1, 0] = back.astype(BF).reshape(share, rows, cols)
    out_ref[:, 0, 0] = total.astype(BF).reshape(groups, rows, cols)


def triangle(at, sides, grads):
    groups, _, per, rows, cols = sides.shape
    side_spec = pl.BlockSpec((groups, 2, 1, rows, cols), lambda c, at: (0, 0, c, 0, 0))
    grad_spec = pl.BlockSpec((groups, 1, rows, cols), lambda c, at: (0, c, 0, 0))
    return pl.pallas_call(
        triangle_kernel,
        grid_spec=pltpu.PrefetchScalarGridSpec(
            num_scalar_prefetch=1,
            grid=(per,),
            in_specs=[side_spec] + [grad_spec] * len(grads),
            out_specs=side_spec,
        ),
        out_shape=jax.ShapeDtypeStruct(sides.shape, BF),
        cost_estimate=pl.CostEstimate(flops=4 * 10**9, bytes_accessed=5 * 2**20, transcendentals=0),
        name="triangle",
    )(at, sides, *grads)


def gate_kernel(in_ref, factors_ref, normed_ref, w_ref, out_ref, raw_ref, flat):
    groups, _, per, rows, _ = in_ref.shape
    half = groups * per
    for g in range(groups):
        for side in range(2):
            for c in range(per):
                first = (side * half + g * per + c) * rows
                flat[first : first + rows, :] = in_ref[g, side, c].astype(F32)

    @pl.when(pl.program_id(0) == 0)
    def _():
        raw_ref[...] = jnp.zeros_like(raw_ref)

    w = w_ref[...]

    def pair(i2, carry):
        made = []
        for e in range(2):
            i = i2 * 2 + e
            parts = []
            for side in range(2):
                incoming = flat[pl.ds(side * half * rows + i, half, stride=rows), :]
                at = 2 * side * half
                parts.append((incoming * factors_ref[i, at : at + half, :]).astype(BF))
                parts.append((incoming * factors_ref[i, at + half : at + 2 * half, :]).astype(BF))
            grads = jnp.concatenate(parts, axis=0)
            made.append(grads)
            back = lax.dot_general(grads, w, (((0,), (0,)), ((), ())), preferred_element_type=F32)
            out_ref[i] = back.astype(BF)
        both = jnp.concatenate(made, axis=1)
        cols, depth = normed_ref.shape[1:]
        normed = normed_ref[pl.ds(i2 * 2, 2)].reshape(2 * cols, depth)
        raw_ref[...] += jnp.dot(both, normed, preferred_element_type=F32)
        return carry

    lax.fori_loop(0, rows // 2, pair, 0)


def gate(incoming, factors, normed, w, step):
    groups, _, per, rows, cols = incoming.shape
    depth = normed.shape[-1]
    return pl.pallas_call(
        gate_kernel,
        grid=(rows // step,),
        in_specs=[
            pl.BlockSpec((groups, 2, per, step, cols), lambda r: (0, 0, 0, r, 0)),
            pl.BlockSpec((step,) + factors.shape[1:], lambda r: (r, 0, 0)),
            pl.BlockSpec((step, cols, depth), lambda r: (r, 0, 0)),
            pl.BlockSpec(w.shape, lambda r: (0, 0)),
        ],
        out_specs=[
            pl.BlockSpec((step, cols, depth), lambda r: (r, 0, 0)),
            pl.BlockSpec(w.shape, lambda r: (0, 0)),
        ],
        out_shape=[
            jax.ShapeDtypeStruct((rows, cols, depth), BF),
            jax.ShapeDtypeStruct(w.shape, F32),
        ],
        scratch_shapes=[pltpu.VMEM((2 * groups * per * step, cols), F32)],
        cost_estimate=pl.CostEstimate(flops=6 * 10**9, bytes_accessed=8 * 2**20, transcendentals=0),
        name="gate",
    )(incoming, factors, normed, w)


def finish_kernel(x_ref, gain_ref, own_ref, other_ref, out_ref):
    unit, inv_std = normalised(x_ref[...].astype(F32))
    scaled = (own_ref[...].astype(F32) + other_ref[...].astype(F32)) * gain_ref[...]
    mean = jnp.mean(scaled, axis=-1, keepdims=True)
    along = jnp.mean(scaled * unit, axis=-1, keepdims=True)
    out_ref[...] = (inv_std * (scaled - mean - unit * along)).astype(BF)


def finish(x, gain, own, other, step):
    rows, cols, depth = x.shape
    spec = pl.BlockSpec((step, cols, depth), lambda r: (r, 0, 0))
    return pl.pallas_call(
        finish_kernel,
        grid=(rows // step,),
        in_specs=[spec, pl.BlockSpec((1, 1, depth), lambda r: (0, 0, 0)), spec, spec],
        out_specs=spec,
        out_shape=jax.ShapeDtypeStruct(x.shape, BF),
        cost_estimate=pl.CostEstimate(flops=10**7, bytes_accessed=4 * 2**20, transcendentals=0),
        name="finish",
    )(x, gain.reshape(1, 1, depth), own, other)


def swapped(x, axis, bit):
    size = lax.axis_size(axis)
    return lax.ppermute(x, axis, [(i, i ^ bit) for i in range(size)])


def on_device(pair_rep, norm_gain, weights, residue_mask, product_grad):
    rows, cols, depth = pair_rep.shape
    chans = product_grad.shape[1]
    groups = lax.axis_size("ia")
    per = chans // groups
    here = lax.axis_index("ja")
    validity = residue_mask.astype(F32)
    row_valid = lax.dynamic_slice_in_dim(validity, lax.axis_index("ia") * rows, rows)
    col_valid = lax.dynamic_slice_in_dim(validity, here * cols, cols)
    pair_valid = row_valid[:, None] * col_valid[None, :]
    w = jnp.swapaxes(weights, 1, 2).reshape(4 * chans, depth)

    grads = channels_first(product_grad).reshape(groups, per, rows, cols)
    grads = lax.all_to_all(grads, "ia", 0, 0, tiled=True)
    sides, factors, normed = project(pair_rep, norm_gain[None], w, pair_valid, groups, 16)
    grads, sides = lax.optimization_barrier((grads, sides))
    far = swapped(grads, "ja", 2)
    sides = lax.all_to_all(sides, "ia", 0, 0, tiled=True)
    near = swapped(grads, "ja", 1)
    farther = swapped(far, "ja", 1)
    at = jnp.stack([here, here ^ 1, here ^ 2, here ^ 3]).astype(jnp.int32)
    products = triangle(at, sides, (grads, near, far, farther))
    products = lax.all_to_all(products, "ia", 0, 0, tiled=True)
    own, raw = gate(products, factors, normed, w, 16)
    raw = raw + swapped(raw, "ja", 2)
    other = swapped(own, "col", 1)
    raw = raw + swapped(raw, "ja", 1)
    pieces = lax.all_to_all(raw.reshape(groups, -1, depth), "ia", 0, 0, tiled=True)
    piece = jnp.sum(pieces, axis=0)
    whole = lax.all_to_all(jnp.broadcast_to(piece[None], pieces.shape), "ia", 0, 0, tiled=True)
    whole = whole.reshape(4, chans, depth)
    squares = jnp.sum(whole * whole).reshape(1, 1)
    squares = squares + swapped(squares, "col", 1)
    factor = jnp.minimum(1.0, CLIP_LIMIT * lax.rsqrt(squares[0, 0] + 1e-06))
    weight_grads = jnp.swapaxes(whole, 1, 2) * factor
    pair_grad = finish(pair_rep, norm_gain, own, other, 8)
    return (pair_grad, weight_grads)


def solution(mesh):
    placed = (P("ia", "ja", None), P(), P(None, None, "col"), P(), P("ia", "col", "ja"))
    return jax.shard_map(
        on_device,
        mesh=mesh,
        in_specs=placed,
        out_specs=(P("ia", "ja", None), P(None, None, "col")),
        check_vma=False,
    )
```

```python
import jax
import jax.numpy as jnp
from jax import lax
from jax.experimental import pallas as pl
from jax.experimental.pallas import tpu as pltpu
from jax.sharding import PartitionSpec as P


CLIP_LIMIT = 64.0
BF, F32 = jnp.bfloat16, jnp.float32
NN = (((1,), (0,)), ((), ()))
NT = (((1,), (1,)), ((), ()))
TN = (((0,), (0,)), ((), ()))
KEPT = pl.BlockSpec(memory_space=pltpu.VMEM)
SCALARS = pl.BlockSpec(memory_space=pltpu.SMEM)
MIB = 2**20


def dot(a, b, dims=NN):
    return lax.dot_general(a, b, dims, preferred_element_type=F32)


def kept(x):
    return pltpu.with_memory_space_constraint(x, pltpu.VMEM)


def in_vmem(shape, dtype):
    return pltpu.VMEM(shape, dtype)


def identity(size):
    row = lax.broadcasted_iota(jnp.int32, (size, size), 0)
    col = lax.broadcasted_iota(jnp.int32, (size, size), 1)
    return (row == col).astype(F32)


def local(kernel, out_shape, args, scratch, specs=None, flops=10**6, moved=MIB, limit=24):
    return pl.pallas_call(
        kernel,
        out_shape=out_shape,
        in_specs=specs or [KEPT] * len(args),
        out_specs=jax.tree.map(lambda _: KEPT, out_shape),
        scratch_shapes=scratch,
        compiler_params=pltpu.CompilerParams(vmem_limit_bytes=limit * MIB),
        cost_estimate=pl.CostEstimate(flops=flops, bytes_accessed=moved, transcendentals=0),
    )(*args)


def channels_first_kernel(x_ref, out_ref, flat):
    rows, chans, width = x_ref.shape
    flat[...] = x_ref[...].reshape(rows * chans, width).astype(F32)
    for c in range(chans):
        out_ref[c] = flat[pl.ds(c, rows, stride=chans), :].astype(BF)


def channels_first(x):
    rows, chans, width = x.shape
    out = in_vmem((chans, rows, width), BF)
    scratch = [pltpu.VMEM((rows * chans, width), F32)]
    return local(channels_first_kernel, out, [kept(x)], scratch, limit=8)


def project_kernel(axes, unroll, x_ref, gain_ref, w_ref, mask_ref, cols_ref, sides_ref, factors_ref, normed_ref, unit_ref, inv_ref, flat):
    rows, cols, depth = x_ref.shape
    groups, _, per, _, _ = sides_ref.shape
    half = groups * per
    first_row = lax.axis_index(axes[0]) * rows
    centring = (identity(depth) - 1.0 / depth).astype(BF)
    gain = jnp.concatenate([gain_ref[...]] * 2, axis=1)
    w = w_ref[...]
    valid_cols = cols_ref[pl.ds(lax.axis_index(axes[1]), 1), :].astype(F32)

    def pair(p, carry):
        x = x_ref[pl.ds(2 * p, 2)].reshape(2 * cols, depth)
        centred = dot(centring, x, NT)
        inv_std = lax.rsqrt(jnp.mean(centred * centred, axis=0, keepdims=True) + 1e-05)
        unit = centred * inv_std
        normed = (unit * gain).astype(BF)
        unit_ref[p] = unit
        inv_ref[pl.ds(p, 1), :] = inv_std
        normed_ref[p] = normed
        proj = dot(w, normed)
        valid = jnp.concatenate([valid_cols * mask_ref[first_row + 2 * p + e].astype(F32) for e in range(2)], axis=1)
        for side in range(2):
            at = 2 * side * half
            linear = proj[at : at + half]
            gate = jax.nn.sigmoid(proj[at + half : at + 2 * half])
            first = valid * gate
            both = first * linear
            for e in range(2):
                put = pl.multiple_of((2 * p + e) * 2 * half + side * half, half)
                flat[pl.ds(put, half), :] = both[:, e * cols : (e + 1) * cols]
            factors_ref[p, at : at + half, :] = first
            factors_ref[p, at + half : at + 2 * half, :] = both * (1.0 - gate)
        return carry

    lax.fori_loop(0, rows // 2, pair, 0, unroll=unroll)
    for g in range(groups):
        for side in range(2):
            for c in range(per):
                first = side * half + g * per + c
                sides_ref[g, side, c] = flat[pl.ds(first, rows, stride=2 * half), :].astype(BF)


def project(x, gain, w, mask, groups, axes=("ia", "ja"), unroll=2):
    rows, cols, depth = x.shape
    half = w.shape[0] // 4
    per = half // groups
    out = [
        in_vmem((groups, 2, per, rows, cols), BF),
        in_vmem((rows // 2, 4 * half, 2 * cols), F32),
        in_vmem((rows // 2, depth, 2 * cols), BF),
        in_vmem((rows // 2, depth, 2 * cols), F32),
        in_vmem((rows // 2, 2 * cols), F32),
    ]
    args = [kept(x), kept(gain), kept(w), mask, kept(mask.reshape(-1, cols))]
    return local(
        lambda *refs: project_kernel(axes, unroll, *refs),
        out,
        args,
        [pltpu.VMEM((rows * 2 * half, cols), F32)],
        specs=[KEPT, KEPT, KEPT, SCALARS, KEPT],
        flops=6 * 10**9,
        moved=8 * MIB,
    )


def triangle_kernel(axis, sides_ref, *refs):
    *grads, out_ref = refs
    groups, _, per, rows, cols = sides_ref.shape
    share = groups // len(grads)
    here = lax.axis_index(axis)
    for c in range(per):
        left = sides_ref[:, 0, c].reshape(groups * rows, cols)
        total = None
        for t, grad_ref in enumerate(grads):
            first = (here ^ t) * share
            grad = grad_ref[:, c].reshape(groups * rows, cols)
            right = sides_ref[pl.ds(first, share), 1, c].reshape(share * rows, cols)
            part = dot(grad, right)
            total = part if total is None else total + part
            back = dot(grad, left, TN)
            out_ref[pl.ds(first, share), 1, c] = back.astype(BF).reshape(share, rows, cols)
        out_ref[:, 0, c] = total.astype(BF).reshape(groups, rows, cols)


def triangle(sides, grads, axis="ja"):
    return local(
        lambda *refs: triangle_kernel(axis, *refs),
        in_vmem(sides.shape, BF),
        [kept(sides)] + [kept(g) for g in grads],
        [],
        flops=4 * 10**9,
        moved=5 * MIB,
    )


def gate_kernel(unroll, in_ref, factors_ref, normed_ref, w_ref, out_ref, raw_ref, flat):
    groups, _, per, rows, _ = in_ref.shape
    half = groups * per
    for g in range(groups):
        for side in range(2):
            for c in range(per):
                first = (side * half + g * per + c) * rows
                flat[first : first + rows, :] = in_ref[g, side, c].astype(F32)
    raw_ref[...] = jnp.zeros_like(raw_ref)
    w = w_ref[...]

    def pair(p, carry):
        parts = []
        for side in range(2):
            incoming = jnp.concatenate(
                [flat[pl.ds(side * half * rows + 2 * p + e, half, stride=rows), :] for e in range(2)], axis=1
            )
            at = 2 * side * half
            parts.append((incoming * factors_ref[p, at : at + half, :]).astype(BF))
            parts.append((incoming * factors_ref[p, at + half : at + 2 * half, :]).astype(BF))
        grads = jnp.concatenate(parts, axis=0)
        raw_ref[...] += dot(grads, normed_ref[p], NT)
        out_ref[p] = dot(w, grads).astype(BF)
        return carry

    lax.fori_loop(0, rows // 2, pair, 0, unroll=unroll)


def gate(incoming, factors, normed, w, unroll=2):
    groups, _, per, rows, cols = incoming.shape
    out = [in_vmem(normed.shape, BF), in_vmem((w.shape[1], w.shape[0]), F32)]
    return local(
        lambda *refs: gate_kernel(unroll, *refs),
        out,
        [kept(a) for a in (incoming, factors, normed, w)],
        [pltpu.VMEM((2 * groups * per * rows, cols), F32)],
        flops=6 * 10**9,
        moved=8 * MIB,
    )


def finish_kernel(unit_ref, inv_ref, gain_ref, own_ref, other_ref, out_ref):
    step, cols, _ = out_ref.shape
    turn = identity(cols).astype(BF)
    gain = jnp.concatenate([gain_ref[...]] * 2, axis=1)
    base = pl.program_id(0) * (step // 2)
    for q in range(step // 2):
        p = base + q
        unit = unit_ref[p]
        scaled = (own_ref[p].astype(F32) + other_ref[p].astype(F32)) * gain
        mean = jnp.mean(scaled, axis=0, keepdims=True)
        along = jnp.mean(scaled * unit, axis=0, keepdims=True)
        made = (inv_ref[pl.ds(p, 1), :] * (scaled - mean - unit * along)).astype(BF)
        for e in range(2):
            out_ref[2 * q + e] = dot(turn, made[:, e * cols : (e + 1) * cols], NT).astype(BF)


def finish(unit, inv_std, gain, own, other, step):
    pairs, depth, twice = unit.shape
    shape = (2 * pairs, twice // 2, depth)
    return pl.pallas_call(
        finish_kernel,
        grid=(shape[0] // step,),
        in_specs=[KEPT] * 5,
        out_specs=pl.BlockSpec((step,) + shape[1:], lambda r: (r, 0, 0)),
        out_shape=jax.ShapeDtypeStruct(shape, BF),
        compiler_params=pltpu.CompilerParams(vmem_limit_bytes=16 * MIB),
        cost_estimate=pl.CostEstimate(flops=10**9, bytes_accessed=4 * MIB, transcendentals=0),
        name="finish",
    )(*[kept(a) for a in (unit, inv_std, gain, own, other)])


def swapped(x, axis, bit):
    size = lax.axis_size(axis)
    return lax.ppermute(x, axis, [(i, i ^ bit) for i in range(size)])


def on_device(pair_rep, norm_gain, weights, residue_mask, product_grad):
    rows, cols, depth = pair_rep.shape
    chans = product_grad.shape[1]
    groups = lax.axis_size("ia")
    per = chans // groups
    w = jnp.swapaxes(weights, 1, 2).reshape(4 * chans, depth)
    w_back = jnp.swapaxes(w, 0, 1)
    gain = jnp.broadcast_to(norm_gain[:, None], (depth, cols))

    grads = channels_first(product_grad).reshape(groups, per, rows, cols)
    grads = lax.all_to_all(grads, "ia", 0, 0, tiled=True)
    sides, factors, normed, unit, inv_std = project(pair_rep, gain, w, residue_mask, groups)
    grads, sides = lax.optimization_barrier((grads, sides))
    far = swapped(grads, "ja", 2)
    sides = lax.all_to_all(sides, "ia", 0, 0, tiled=True)
    near = swapped(grads, "ja", 1)
    farther = swapped(far, "ja", 1)
    products = triangle(sides, (grads, near, far, farther))
    products = lax.all_to_all(products, "ia", 0, 0, tiled=True)
    own, raw = gate(products, factors, normed, w_back)
    raw = raw + swapped(raw, "ja", 2)
    other = swapped(own, "col", 1)
    raw = raw + swapped(raw, "ja", 1)
    pieces = lax.all_to_all(raw.reshape(groups, -1, depth), "ia", 0, 0, tiled=True)
    piece = jnp.sum(pieces, axis=0)
    whole = lax.all_to_all(jnp.broadcast_to(piece[None], pieces.shape), "ia", 0, 0, tiled=True)
    whole = whole.reshape(4, chans, depth)
    squares = jnp.sum(whole * whole).reshape(1, 1)
    others = swapped(squares, "col", 1)
    pair_grad = finish(unit, inv_std, gain, own, other, 8)
    others, pair_grad = lax.optimization_barrier((others, pair_grad))
    factor = jnp.minimum(1.0, CLIP_LIMIT * lax.rsqrt((squares + others)[0, 0] + 1e-06))
    weight_grads = jnp.swapaxes(whole, 1, 2) * factor
    return (pair_grad, weight_grads)


def solution(mesh):
    placed = (P("ia", "ja", None), P(), P(None, None, "col"), P(), P("ia", "col", "ja"))
    return jax.shard_map(
        on_device,
        mesh=mesh,
        in_specs=placed,
        out_specs=(P("ia", "ja", None), P(None, None, "col")),
        check_vma=False,
    )
```

```python
import jax
import jax.numpy as jnp
from jax import lax
from jax.experimental import pallas as pl
from jax.experimental.pallas import tpu as pltpu
from jax.sharding import PartitionSpec as P


CLIP_LIMIT = 64.0
BF, F32 = jnp.bfloat16, jnp.float32
NN = (((1,), (0,)), ((), ()))
NT = (((1,), (1,)), ((), ()))
TN = (((0,), (0,)), ((), ()))
KEPT = pl.BlockSpec(memory_space=pltpu.VMEM)
SCALARS = pl.BlockSpec(memory_space=pltpu.SMEM)
MIB = 2**20


def dot(a, b, dims=NN):
    return lax.dot_general(a, b, dims, preferred_element_type=F32)


def kept(x):
    return pltpu.with_memory_space_constraint(x, pltpu.VMEM)


def in_hbm(x):
    return pltpu.with_memory_space_constraint(x, pltpu.HBM)


def identity(size):
    row = lax.broadcasted_iota(jnp.int32, (size, size), 0)
    col = lax.broadcasted_iota(jnp.int32, (size, size), 1)
    return (row == col).astype(F32)


def call(kernel, out_shape, args, in_specs, out_specs, scratch=(), grid=(), flops=10**6, moved=MIB):
    return pl.pallas_call(
        kernel,
        grid=grid,
        out_shape=out_shape,
        in_specs=in_specs,
        out_specs=out_specs,
        scratch_shapes=list(scratch),
        compiler_params=pltpu.CompilerParams(vmem_limit_bytes=24 * MIB),
        cost_estimate=pl.CostEstimate(flops=flops, bytes_accessed=moved, transcendentals=0),
    )(*args)


def fixed(shape):
    return pl.BlockSpec(shape, lambda r: (0,) * len(shape))


def leading(step, shape):
    return pl.BlockSpec((step,) + tuple(shape[1:]), lambda r: (r,) + (0,) * (len(shape) - 1))


def channels_first_kernel(x_ref, out_ref, flat):
    rows, chans, width = x_ref.shape
    flat[...] = x_ref[...].reshape(rows * chans, width).astype(F32)
    for c in range(chans):
        out_ref[c] = flat[pl.ds(c, rows, stride=chans), :].astype(BF)


def channels_first(x, step=16):
    rows, chans, width = x.shape
    return call(
        channels_first_kernel,
        jax.ShapeDtypeStruct((chans, rows, width), BF),
        [x],
        [leading(step, x.shape)],
        pl.BlockSpec((chans, step, width), lambda r: (0, r, 0)),
        [pltpu.VMEM((step * chans, width), F32)],
        (rows // step,),
    )


def project_kernel(axes, unroll, x_ref, gain_ref, w_ref, mask_ref, cols_ref, sides_ref, factors_ref, normed_ref, unit_ref, inv_ref, flat, gains):
    rows, cols, depth = x_ref.shape
    groups, _, per, _, _ = sides_ref.shape
    half = groups * per
    step = pl.program_id(0)
    first_row = lax.axis_index(axes[0]) * (rows * pl.num_programs(0)) + step * rows
    centring = (identity(depth) - 1.0 / depth).astype(BF)

    @pl.when(step == 0)
    def _():
        gains[...] = jnp.broadcast_to(gain_ref[...], (2 * cols, depth)).T

    w = w_ref[...]
    valid_cols = cols_ref[pl.ds(lax.axis_index(axes[1]), 1), :].astype(F32)

    def pair(p, carry):
        x = x_ref[pl.ds(2 * p, 2)].reshape(2 * cols, depth)
        centred = dot(centring, x, NT)
        inv_std = lax.rsqrt(jnp.mean(centred * centred, axis=0, keepdims=True) + 1e-05)
        unit = centred * inv_std
        normed = (unit * gains[...]).astype(BF)
        unit_ref[p] = unit
        inv_ref[p] = inv_std
        whole = step * (rows // 2) + p
        normed_ref[whole] = normed
        proj = dot(w, normed)
        valid = jnp.concatenate([valid_cols * mask_ref[first_row + 2 * p + e].astype(F32) for e in range(2)], axis=1)
        for side in range(2):
            at = 2 * side * half
            linear = proj[at : at + half]
            gate = jax.nn.sigmoid(proj[at + half : at + 2 * half])
            first = valid * gate
            both = first * linear
            for e in range(2):
                put = pl.multiple_of((2 * p + e) * 2 * half + side * half, half)
                flat[pl.ds(put, half), :] = both[:, e * cols : (e + 1) * cols]
            factors_ref[whole, at : at + half, :] = first.astype(BF)
            factors_ref[whole, at + half : at + 2 * half, :] = (both * (1.0 - gate)).astype(BF)
        return carry

    lax.fori_loop(0, rows // 2, pair, 0, unroll=unroll)
    for g in range(groups):
        for side in range(2):
            for c in range(per):
                first = side * half + g * per + c
                sides_ref[g, side, c] = flat[pl.ds(first, rows, stride=2 * half), :].astype(BF)


def project(x, gain, w, mask, groups, axes=("ia", "ja"), unroll=8, step=16):
    rows, cols, depth = x.shape
    half = w.shape[0] // 4
    per = half // groups
    pairs = rows // 2
    out = [
        pltpu.HBM((groups, 2, per, rows, cols), BF),
        pltpu.VMEM((pairs, 4 * half, 2 * cols), BF),
        pltpu.VMEM((pairs, depth, 2 * cols), BF),
        pltpu.HBM((pairs, depth, 2 * cols), F32),
        pltpu.HBM((pairs, 1, 2 * cols), F32),
    ]
    table = mask.reshape(-1, cols)
    return call(
        lambda *refs: project_kernel(axes, unroll, *refs),
        out,
        [in_hbm(x), in_hbm(gain[None]), in_hbm(w), mask, in_hbm(table)],
        [leading(step, x.shape), fixed((1, depth)), fixed(w.shape), SCALARS, fixed(table.shape)],
        [pl.BlockSpec((groups, 2, per, step, cols), lambda r: (0, 0, 0, r, 0))] + [KEPT, KEPT] + [leading(step // 2, o.shape) for o in out[3:]],
        [pltpu.VMEM((step * 2 * half, cols), F32), pltpu.VMEM((depth, 2 * cols), F32)],
        (rows // step,),
        flops=6 * 10**9,
        moved=8 * MIB,
    )


def triangle_kernel(axis, sides_ref, *refs):
    *grads, out_ref = refs
    groups, _, per, rows, cols = sides_ref.shape
    share = groups // len(grads)
    here = lax.axis_index(axis)
    for c in range(per):
        left = sides_ref[:, 0, c].reshape(groups * rows, cols)
        total = None
        for t, grad_ref in enumerate(grads):
            first = (here ^ t) * share
            grad = grad_ref[:, c].reshape(groups * rows, cols)
            right = sides_ref[pl.ds(first, share), 1, c].reshape(share * rows, cols)
            part = dot(grad, right)
            total = part if total is None else total + part
            back = dot(grad, left, TN)
            out_ref[pl.ds(first, share), 1, c] = back.astype(BF).reshape(share, rows, cols)
        out_ref[:, 0, c] = total.astype(BF).reshape(groups, rows, cols)


def triangle(sides, grads, axis="ja"):
    return call(
        lambda *refs: triangle_kernel(axis, *refs),
        pltpu.HBM(sides.shape, BF),
        [kept(sides)] + [in_hbm(g) for g in grads],
        [KEPT] * (1 + len(grads)),
        KEPT,
        flops=4 * 10**9,
        moved=5 * MIB,
    )


def gate_kernel(unroll, in_ref, factors_ref, normed_ref, w_ref, out_ref, raw_ref, flat):
    groups, _, per, rows, _ = in_ref.shape
    half = groups * per
    pairs = out_ref.shape[0]
    step = pl.program_id(0)

    @pl.when(step == 0)
    def _():
        for g in range(groups):
            for side in range(2):
                for c in range(per):
                    first = (side * half + g * per + c) * rows
                    flat[first : first + rows, :] = in_ref[g, side, c].astype(F32)
        raw_ref[...] = jnp.zeros_like(raw_ref)

    w = w_ref[...].T

    def pair(q, carry):
        p = step * pairs + q
        parts = []
        for side in range(2):
            incoming = jnp.concatenate(
                [flat[pl.ds(side * half * rows + 2 * p + e, half, stride=rows), :] for e in range(2)], axis=1
            )
            at = 2 * side * half
            for first in (at, at + half):
                parts.append((incoming * factors_ref[p, first : first + half, :].astype(F32)).astype(BF))
        grads = jnp.concatenate(parts, axis=0)
        raw_ref[...] += dot(grads, normed_ref[p], NT)
        out_ref[q] = dot(w, grads).astype(BF)
        return carry

    lax.fori_loop(0, pairs, pair, 0, unroll=unroll)


def gate(incoming, factors, normed, w, unroll=8, step=8):
    groups, _, per, rows, cols = incoming.shape
    return call(
        lambda *refs: gate_kernel(unroll, *refs),
        [pltpu.HBM(normed.shape, BF), jax.ShapeDtypeStruct(w.shape, F32)],
        [kept(incoming), kept(factors), kept(normed), in_hbm(w)],
        [KEPT, KEPT, KEPT, fixed(w.shape)],
        [leading(step, normed.shape), fixed(w.shape)],
        [pltpu.VMEM((2 * groups * per * rows, cols), F32)],
        (normed.shape[0] // step,),
        flops=6 * 10**9,
        moved=8 * MIB,
    )


def finish_kernel(unit_ref, inv_ref, gain_ref, own_ref, other_ref, out_ref, gains):
    step, cols, depth = out_ref.shape

    @pl.when(pl.program_id(0) == 0)
    def _():
        gains[...] = jnp.broadcast_to(gain_ref[...], (2 * cols, depth)).T

    turn = identity(2 * cols).astype(BF)
    base = pl.program_id(0) * (step // 2)
    for q in range(step // 2):
        unit = unit_ref[q]
        scaled = (own_ref[q].astype(F32) + other_ref[base + q].astype(F32)) * gains[...]
        mean = jnp.mean(scaled, axis=0, keepdims=True)
        along = jnp.mean(scaled * unit, axis=0, keepdims=True)
        made = (inv_ref[q] * (scaled - mean - unit * along)).astype(BF)
        out_ref[pl.ds(2 * q, 2)] = dot(turn, made, NT).astype(BF).reshape(2, cols, depth)


def finish(unit, inv_std, gain, own, other, step=16):
    pairs, depth, twice = unit.shape
    shape = (2 * pairs, twice // 2, depth)
    half = step // 2
    return call(
        finish_kernel,
        jax.ShapeDtypeStruct(shape, BF),
        [in_hbm(unit), in_hbm(inv_std), in_hbm(gain[None]), in_hbm(own), kept(other)],
        [leading(half, unit.shape), leading(half, inv_std.shape), fixed((1, depth)), leading(half, own.shape), KEPT],
        leading(step, shape),
        [pltpu.VMEM((depth, twice), F32)],
        (shape[0] // step,),
        flops=10**9,
        moved=4 * MIB,
    )


def scale_kernel(whole_ref, mine_ref, others_ref, out_ref):
    factor = jnp.minimum(1.0, CLIP_LIMIT * lax.rsqrt(mine_ref[...] + others_ref[...] + 1e-06))
    out_ref[...] = whole_ref[...] * factor


def scale(whole, mine, others):
    return call(scale_kernel, pltpu.HBM(whole.shape, F32), [kept(whole), mine, others], [KEPT] * 3, KEPT)


def swapped(x, axis, bit):
    size = lax.axis_size(axis)
    return lax.ppermute(x, axis, [(i, i ^ bit) for i in range(size)])


def on_device(pair_rep, norm_gain, weights, residue_mask, product_grad):
    rows, cols, depth = pair_rep.shape
    chans = product_grad.shape[1]
    groups = lax.axis_size("ia")
    per = chans // groups
    w = jnp.swapaxes(weights, 1, 2).reshape(4 * chans, depth)

    grads = channels_first(product_grad).reshape(groups, per, rows, cols)
    grads = lax.all_to_all(grads, "ia", 0, 0, tiled=True)
    sides, factors, normed, unit, inv_std = project(pair_rep, norm_gain, w, residue_mask, groups)
    grads, sides = lax.optimization_barrier((grads, sides))
    far = swapped(grads, "ja", 2)
    sides = lax.all_to_all(sides, "ia", 0, 0, tiled=True)
    near = swapped(grads, "ja", 1)
    farther = swapped(far, "ja", 1)
    products = triangle(sides, (grads, near, far, farther))
    products = lax.all_to_all(products, "ia", 0, 0, tiled=True)
    own, raw = gate(products, factors, normed, w)
    raw = raw + swapped(raw, "ja", 2)
    other = swapped(own, "col", 1)
    raw = raw + swapped(raw, "ja", 1)
    pieces = lax.all_to_all(raw.reshape(groups, -1, depth), "ia", 0, 0, tiled=True)
    piece = jnp.sum(pieces, axis=0)
    whole = lax.all_to_all(jnp.broadcast_to(piece[None], pieces.shape), "ia", 0, 0, tiled=True)
    whole = whole.reshape(4 * chans, depth)
    squares = jnp.sum(whole * whole).reshape(1, 1)
    others = swapped(squares, "col", 1)
    pair_grad = finish(unit, inv_std, norm_gain, own, other)
    others, pair_grad = lax.optimization_barrier((others, pair_grad))
    weight_grads = jnp.swapaxes(scale(whole, squares, others).reshape(4, chans, depth), 1, 2)
    return (pair_grad, weight_grads)


def solution(mesh):
    placed = (P("ia", "ja", None), P(), P(None, None, "col"), P(), P("ia", "col", "ja"))
    return jax.shard_map(
        on_device,
        mesh=mesh,
        in_specs=placed,
        out_specs=(P("ia", "ja", None), P(None, None, "col")),
        check_vma=False,
    )
```

```python
import jax
import jax.numpy as jnp
from jax import lax
from jax.experimental import pallas as pl
from jax.experimental.pallas import tpu as pltpu
from jax.sharding import Mesh
from jax.sharding import PartitionSpec as P


CLIP_LIMIT = 64.0
BF, F32 = jnp.bfloat16, jnp.float32
NN = (((1,), (0,)), ((), ()))
NT = (((1,), (1,)), ((), ()))
TN = (((0,), (0,)), ((), ()))
KEPT = pl.BlockSpec(memory_space=pltpu.VMEM)
SCALARS = pl.BlockSpec(memory_space=pltpu.SMEM)
MIB = 2**20


def dot(a, b, dims=NN):
    return lax.dot_general(a, b, dims, preferred_element_type=F32)


def kept(x):
    return pltpu.with_memory_space_constraint(x, pltpu.VMEM)


def in_hbm(x):
    return pltpu.with_memory_space_constraint(x, pltpu.HBM)


def identity(size):
    row = lax.broadcasted_iota(jnp.int32, (size, size), 0)
    col = lax.broadcasted_iota(jnp.int32, (size, size), 1)
    return (row == col).astype(F32)


def call(kernel, out_shape, args, in_specs, out_specs, scratch=(), grid=(), flops=10**6, moved=MIB):
    return pl.pallas_call(
        kernel,
        grid=grid,
        out_shape=out_shape,
        in_specs=in_specs,
        out_specs=out_specs,
        scratch_shapes=list(scratch),
        compiler_params=pltpu.CompilerParams(vmem_limit_bytes=24 * MIB),
        cost_estimate=pl.CostEstimate(flops=flops, bytes_accessed=moved, transcendentals=0),
    )(*args)


def fixed(shape):
    return pl.BlockSpec(shape, lambda r: (0,) * len(shape))


def leading(step, shape):
    return pl.BlockSpec((step,) + tuple(shape[1:]), lambda r: (r,) + (0,) * (len(shape) - 1))


def channels_first_kernel(x_ref, out_ref, flat):
    rows, chans, width = x_ref.shape
    flat[...] = x_ref[...].reshape(rows * chans, width).astype(F32)
    for c in range(chans):
        out_ref[c] = flat[pl.ds(c, rows, stride=chans), :].astype(BF)


def channels_first(x, step=16):
    rows, chans, width = x.shape
    return call(
        channels_first_kernel,
        jax.ShapeDtypeStruct((chans, rows, width), BF),
        [x],
        [leading(step, x.shape)],
        pl.BlockSpec((chans, step, width), lambda r: (0, r, 0)),
        [pltpu.VMEM((step * chans, width), F32)],
        (rows // step,),
    )


def project_kernel(axes, unroll, x_ref, gain_ref, w_ref, mask_ref, cols_ref, sides_ref, factors_ref, normed_ref, unit_ref, inv_ref, flat, gains):
    rows, cols, depth = x_ref.shape
    groups, _, per, _, _ = sides_ref.shape
    half = groups * per
    step = pl.program_id(0)
    first_row = lax.axis_index(axes[0]) * (rows * pl.num_programs(0)) + step * rows
    centring = (identity(depth) - 1.0 / depth).astype(BF)

    @pl.when(step == 0)
    def _():
        gains[...] = jnp.broadcast_to(gain_ref[...], (2 * cols, depth)).T

    w = w_ref[...]
    valid_cols = cols_ref[pl.ds(lax.axis_index(axes[1]), 1), :].astype(F32)

    def pair(p, carry):
        x = x_ref[pl.ds(2 * p, 2)].reshape(2 * cols, depth)
        centred = dot(centring, x, NT)
        inv_std = lax.rsqrt(jnp.mean(centred * centred, axis=0, keepdims=True) + 1e-05)
        unit = centred * inv_std
        normed = (unit * gains[...]).astype(BF)
        unit_ref[p] = unit
        inv_ref[p] = inv_std
        whole = step * (rows // 2) + p
        normed_ref[p] = normed
        proj = dot(w, normed)
        valid = jnp.concatenate([valid_cols * mask_ref[first_row + 2 * p + e].astype(F32) for e in range(2)], axis=1)
        for side in range(2):
            at = 2 * side * half
            linear = proj[at : at + half]
            gate = jax.nn.sigmoid(proj[at + half : at + 2 * half])
            first = valid * gate
            both = first * linear
            for e in range(2):
                put = pl.multiple_of((2 * p + e) * 2 * half + side * half, half)
                flat[pl.ds(put, half), :] = both[:, e * cols : (e + 1) * cols]
            factors_ref[whole, at : at + half, :] = first.astype(BF)
            factors_ref[whole, at + half : at + 2 * half, :] = (both * (1.0 - gate)).astype(BF)
        return carry

    lax.fori_loop(0, rows // 2, pair, 0, unroll=unroll)
    for g in range(groups):
        for side in range(2):
            for c in range(per):
                first = side * half + g * per + c
                sides_ref[g, side, c] = flat[pl.ds(first, rows, stride=2 * half), :].astype(BF)


def project(x, gain, w, mask, groups, axes=("ia", ("z_lo", "core")), unroll=4, step=8):
    rows, cols, depth = x.shape
    half = w.shape[0] // 4
    per = half // groups
    pairs = rows // 2
    out = [
        pltpu.HBM((groups, 2, per, rows, cols), BF),
        pltpu.VMEM((pairs, 4 * half, 2 * cols), BF),
        pltpu.HBM((pairs, depth, 2 * cols), BF),
        pltpu.HBM((pairs, depth, 2 * cols), F32),
        pltpu.HBM((pairs, 1, 2 * cols), F32),
    ]
    table = mask.reshape(-1, cols)
    return call(
        lambda *refs: project_kernel(axes, unroll, *refs),
        out,
        [in_hbm(x), in_hbm(gain[None]), in_hbm(w), mask, in_hbm(table)],
        [leading(step, x.shape), fixed((1, depth)), fixed(w.shape), SCALARS, fixed(table.shape)],
        [pl.BlockSpec((groups, 2, per, step, cols), lambda r: (0, 0, 0, r, 0))] + [KEPT] + [leading(step // 2, o.shape) for o in out[2:]],
        [pltpu.VMEM((step * 2 * half, cols), F32), pltpu.VMEM((depth, 2 * cols), F32)],
        (rows // step,),
        flops=6 * 10**9,
        moved=8 * MIB,
    )


def triangle_kernel(axis, sides_ref, *refs):
    *grads, out_ref = refs
    groups, _, per, rows, cols = sides_ref.shape
    share = groups // len(grads)
    here = lax.axis_index(axis)
    for c in range(per):
        left = sides_ref[:, 0, c].reshape(groups * rows, cols)
        total = None
        for t, grad_ref in enumerate(grads):
            first = (here ^ t) * share
            grad = grad_ref[:, c].reshape(groups * rows, cols)
            right = sides_ref[pl.ds(first, share), 1, c].reshape(share * rows, cols)
            part = dot(grad, right)
            total = part if total is None else total + part
            back = dot(grad, left, TN)
            out_ref[pl.ds(first, share), 1, c] = back.astype(BF).reshape(share, rows, cols)
        out_ref[:, 0, c] = total.astype(BF).reshape(groups, rows, cols)


def triangle(sides, grads, axis=("z_lo", "core")):
    return call(
        lambda *refs: triangle_kernel(axis, *refs),
        pltpu.HBM(sides.shape, BF),
        [kept(sides)] + [in_hbm(g) for g in grads],
        [KEPT] * (1 + len(grads)),
        KEPT,
        flops=4 * 10**9,
        moved=5 * MIB,
    )


def gate_kernel(unroll, in_ref, factors_ref, normed_ref, w_ref, out_ref, raw_ref, flat, total):
    groups, _, per, rows, _ = in_ref.shape
    half = groups * per
    pairs = normed_ref.shape[0]
    step = pl.program_id(0)

    @pl.when(step == 0)
    def _():
        for g in range(groups):
            for side in range(2):
                for c in range(per):
                    first = (side * half + g * per + c) * rows
                    flat[first : first + rows, :] = in_ref[g, side, c].astype(F32)
        total[...] = jnp.zeros_like(total)

    w = w_ref[...].T

    def pair(q, carry):
        p = step * pairs + q
        parts = []
        for side in range(2):
            incoming = jnp.concatenate(
                [flat[pl.ds(side * half * rows + 2 * p + e, half, stride=rows), :] for e in range(2)], axis=1
            )
            at = 2 * side * half
            for first in (at, at + half):
                parts.append((incoming * factors_ref[p, first : first + half, :].astype(F32)).astype(BF))
        grads = jnp.concatenate(parts, axis=0)
        total[...] += dot(grads, normed_ref[q], NT)
        out_ref[p] = dot(w, grads).astype(BF)
        return carry

    lax.fori_loop(0, pairs, pair, 0, unroll=unroll)

    @pl.when(step == pl.num_programs(0) - 1)
    def _():
        raw_ref[...] = total[...].astype(BF)


def gate(incoming, factors, normed, w, unroll=4, step=4):
    groups, _, per, rows, cols = incoming.shape
    return call(
        lambda *refs: gate_kernel(unroll, *refs),
        [pltpu.VMEM(normed.shape, BF), pltpu.VMEM(w.shape, BF)],
        [kept(incoming), kept(factors), in_hbm(normed), in_hbm(w)],
        [KEPT, KEPT, leading(step, normed.shape), fixed(w.shape)],
        [KEPT, KEPT],
        [pltpu.VMEM((2 * groups * per * rows, cols), F32), pltpu.VMEM(w.shape, F32)],
        (normed.shape[0] // step,),
        flops=6 * 10**9,
        moved=8 * MIB,
    )


def finish_kernel(unit_ref, inv_ref, gain_ref, own_ref, other_ref, out_ref, gains):
    step, cols, depth = out_ref.shape

    @pl.when(pl.program_id(0) == 0)
    def _():
        gains[...] = jnp.broadcast_to(gain_ref[...], (2 * cols, depth)).T

    turn = identity(2 * cols).astype(BF)
    base = pl.program_id(0) * (step // 2)
    for q in range(step // 2):
        unit = unit_ref[q]
        scaled = (own_ref[base + q].astype(F32) + other_ref[base + q].astype(F32)) * gains[...]
        mean = jnp.mean(scaled, axis=0, keepdims=True)
        along = jnp.mean(scaled * unit, axis=0, keepdims=True)
        made = (inv_ref[q] * (scaled - mean - unit * along)).astype(BF)
        out_ref[pl.ds(2 * q, 2)] = dot(turn, made, NT).astype(BF).reshape(2, cols, depth)


def finish(unit, inv_std, gain, own, other, step=16):
    pairs, depth, twice = unit.shape
    shape = (2 * pairs, twice // 2, depth)
    half = step // 2
    return call(
        finish_kernel,
        jax.ShapeDtypeStruct(shape, BF),
        [in_hbm(unit), in_hbm(inv_std), in_hbm(gain[None]), kept(own), kept(other)],
        [leading(half, unit.shape), leading(half, inv_std.shape), fixed((1, depth)), KEPT, KEPT],
        leading(step, shape),
        [pltpu.VMEM((depth, twice), F32)],
        (shape[0] // step,),
        flops=10**9,
        moved=4 * MIB,
    )


def clip_kernel(axis, pieces_ref, out_ref):
    count, rows, depth = pieces_ref.shape
    here = lax.axis_index(axis)
    total = jnp.zeros((rows, depth), F32)
    for n in range(count):
        piece = pieces_ref[n].astype(F32)
        total = total + piece * piece
    squares = jnp.sum(jnp.sum(total, axis=0, keepdims=True), axis=1, keepdims=True)
    factor = jnp.minimum(1.0, CLIP_LIMIT * lax.rsqrt(squares + 1e-06))
    for n in range(count // 2):
        out_ref[n * rows : (n + 1) * rows, :] = pieces_ref[2 * n + here].astype(F32) * factor


def clip(pieces, axis="col"):
    count, rows, depth = pieces.shape
    return call(
        lambda *refs: clip_kernel(axis, *refs),
        pltpu.HBM((count // 2 * rows, depth), F32),
        [kept(pieces)],
        [KEPT],
        KEPT,
    )


def swapped(x, axis):
    return lax.ppermute(x, axis, [(0, 1), (1, 0)])


def on_device(pair_rep, norm_gain, weights, residue_mask, product_grad):
    rows, cols, depth = pair_rep.shape
    chans = product_grad.shape[1]
    groups = lax.axis_size("ia")
    per = chans // groups
    w = jnp.swapaxes(weights, 1, 2).reshape(4 * chans, depth)

    grads = channels_first(product_grad).reshape(groups, per, rows, cols)
    grads = lax.all_to_all(grads, "ia", 0, 0, tiled=True)
    sides, factors, normed, unit, inv_std = project(pair_rep, norm_gain, w, residue_mask, groups)
    grads, sides = lax.optimization_barrier((grads, sides))
    far = swapped(grads, "z_lo")
    sides = lax.all_to_all(sides, "ia", 0, 0, tiled=True)
    near = swapped(grads, "core")
    farther = swapped(far, "core")
    products = triangle(sides, (grads, near, far, farther))
    products = lax.all_to_all(products, "ia", 0, 0, tiled=True)
    own, raw = gate(products, factors, normed, w)
    raw = raw.astype(F32) + swapped(raw, "z_lo").astype(F32)
    other = swapped(own, "col")
    peers = ("ia", "core")
    pieces = raw.reshape(lax.axis_size(peers), -1, depth)
    piece = jnp.sum(lax.all_to_all(pieces, peers, 0, 0, tiled=True), axis=0)
    everyone = ("ia", "core", "col")
    copies = jnp.broadcast_to(piece.astype(BF)[None], (lax.axis_size(everyone),) + piece.shape)
    pieces = lax.all_to_all(copies, everyone, 0, 0, tiled=True)
    pair_grad = finish(unit, inv_std, norm_gain, own, other)
    pieces, pair_grad = lax.optimization_barrier((pieces, pair_grad))
    weight_grads = jnp.swapaxes(clip(pieces).reshape(4, chans, depth), 1, 2)
    return (pair_grad, weight_grads)


def solution(mesh):
    sizes = dict(mesh.shape)
    split = (sizes["ia"], sizes["ja"] // 2, 2, sizes["col"])
    fine = Mesh(mesh.devices.reshape(split), ("ia", "z_lo", "core", "col"))
    ja = ("z_lo", "core")
    return jax.shard_map(
        on_device,
        mesh=fine,
        in_specs=(P("ia", ja, None), P(), P(None, None, "col"), P(), P("ia", "col", ja)),
        out_specs=(P("ia", ja, None), P(None, None, "col")),
        check_vma=False,
    )
```

```python
import jax
import jax.numpy as jnp
from jax import lax
from jax.experimental import pallas as pl
from jax.experimental.pallas import tpu as pltpu
from jax.sharding import Mesh
from jax.sharding import PartitionSpec as P


CLIP_LIMIT = 64.0
BF, F32 = jnp.bfloat16, jnp.float32
NN = (((1,), (0,)), ((), ()))
NT = (((1,), (1,)), ((), ()))
TN = (((0,), (0,)), ((), ()))
KEPT = pl.BlockSpec(memory_space=pltpu.VMEM)
SCALARS = pl.BlockSpec(memory_space=pltpu.SMEM)
MIB = 2**20


def dot(a, b, dims=NN):
    return lax.dot_general(a, b, dims, preferred_element_type=F32)


def kept(x):
    return pltpu.with_memory_space_constraint(x, pltpu.VMEM)


def in_hbm(x):
    return pltpu.with_memory_space_constraint(x, pltpu.HBM)


def identity(size):
    row = lax.broadcasted_iota(jnp.int32, (size, size), 0)
    col = lax.broadcasted_iota(jnp.int32, (size, size), 1)
    return (row == col).astype(F32)


def call(kernel, out_shape, args, in_specs, out_specs, scratch=(), grid=(), flops=10**6, moved=MIB):
    return pl.pallas_call(
        kernel,
        grid=grid,
        out_shape=out_shape,
        in_specs=in_specs,
        out_specs=out_specs,
        scratch_shapes=list(scratch),
        compiler_params=pltpu.CompilerParams(vmem_limit_bytes=24 * MIB),
        cost_estimate=pl.CostEstimate(flops=flops, bytes_accessed=moved, transcendentals=0),
    )(*args)


def fixed(shape):
    return pl.BlockSpec(shape, lambda r: (0,) * len(shape))


def leading(step, shape):
    return pl.BlockSpec((step,) + tuple(shape[1:]), lambda r: (r,) + (0,) * (len(shape) - 1))


def channels_first_kernel(x_ref, out_ref, flat):
    rows, chans, width = x_ref.shape
    flat[...] = x_ref[...].reshape(rows * chans, width).astype(F32)
    for c in range(chans):
        out_ref[c] = flat[pl.ds(c, rows, stride=chans), :].astype(BF)


def channels_first(x, step=16):
    rows, chans, width = x.shape
    return call(
        channels_first_kernel,
        jax.ShapeDtypeStruct((chans, rows, width), BF),
        [x],
        [leading(step, x.shape)],
        pl.BlockSpec((chans, step, width), lambda r: (0, r, 0)),
        [pltpu.VMEM((step * chans, width), F32)],
        (rows // step,),
    )


def project_kernel(axes, unroll, x_ref, gain_ref, w_ref, mask_ref, cols_ref, sides_ref, factors_ref, normed_ref, unit_ref, inv_ref, flat, gains):
    rows, cols, depth = x_ref.shape
    groups, _, per, _, _ = sides_ref.shape
    half = groups * per
    step = pl.program_id(0)
    first_row = lax.axis_index(axes[0]) * (rows * pl.num_programs(0)) + step * rows
    centring = (identity(depth) - 1.0 / depth).astype(BF)

    @pl.when(step == 0)
    def _():
        gains[...] = jnp.broadcast_to(gain_ref[...], (2 * cols, depth)).T

    w = w_ref[...]
    valid_cols = cols_ref[pl.ds(lax.axis_index(axes[1]), 1), :].astype(F32)

    def pair(p, carry):
        x = x_ref[pl.ds(2 * p, 2)].reshape(2 * cols, depth)
        centred = dot(centring, x, NT)
        inv_std = lax.rsqrt(jnp.mean(centred * centred, axis=0, keepdims=True) + 1e-05)
        unit = centred * inv_std
        normed = (unit * gains[...]).astype(BF)
        unit_ref[p] = unit
        inv_ref[p] = inv_std
        normed_ref[p] = normed
        proj = dot(w, normed)
        valid = jnp.concatenate([valid_cols * mask_ref[first_row + 2 * p + e].astype(F32) for e in range(2)], axis=1)
        for side in range(2):
            at = 2 * side * half
            linear = proj[at : at + half]
            gate = jax.nn.sigmoid(proj[at + half : at + 2 * half])
            first = valid * gate
            both = first * linear
            for e in range(2):
                put = pl.multiple_of((2 * p + e) * 2 * half + side * half, half)
                flat[pl.ds(put, half), :] = both[:, e * cols : (e + 1) * cols]
            factors_ref[p, at : at + half, :] = first.astype(BF)
            factors_ref[p, at + half : at + 2 * half, :] = (both * (1.0 - gate)).astype(BF)
        return carry

    lax.fori_loop(0, rows // 2, pair, 0, unroll=unroll)
    for g in range(groups):
        for side in range(2):
            for c in range(per):
                first = side * half + g * per + c
                sides_ref[g, side, c] = flat[pl.ds(first, rows, stride=2 * half), :].astype(BF)


def project(x, gain, w, mask, groups, axes=("ia", ("z_lo", "core")), unroll=4, step=8):
    rows, cols, depth = x.shape
    half = w.shape[0] // 4
    per = half // groups
    pairs = rows // 2
    out = [
        pltpu.HBM((groups, 2, per, rows, cols), BF),
        pltpu.HBM((pairs, 4 * half, 2 * cols), BF),
        pltpu.HBM((pairs, depth, 2 * cols), BF),
        pltpu.HBM((pairs, depth, 2 * cols), F32),
        pltpu.HBM((pairs, 1, 2 * cols), F32),
    ]
    table = mask.reshape(-1, cols)
    return call(
        lambda *refs: project_kernel(axes, unroll, *refs),
        out,
        [in_hbm(x), in_hbm(gain[None]), in_hbm(w), mask, in_hbm(table)],
        [leading(step, x.shape), fixed((1, depth)), fixed(w.shape), SCALARS, fixed(table.shape)],
        [pl.BlockSpec((groups, 2, per, step, cols), lambda r: (0, 0, 0, r, 0))] + [leading(step // 2, o.shape) for o in out[1:]],
        [pltpu.VMEM((step * 2 * half, cols), F32), pltpu.VMEM((depth, 2 * cols), F32)],
        (rows // step,),
        flops=6 * 10**9,
        moved=8 * MIB,
    )


def triangle_kernel(axis, sides_ref, *refs):
    *grads, out_ref = refs
    groups, _, _, rows, cols = sides_ref.shape
    share = groups // len(grads)
    here = lax.axis_index(axis)
    c = pl.program_id(0)
    left = sides_ref[:, 0, c].reshape(groups * rows, cols)
    total = None
    for t, grad_ref in enumerate(grads):
        first = (here ^ t) * share
        grad = grad_ref[:, 0].reshape(groups * rows, cols)
        right = sides_ref[pl.ds(first, share), 1, c].reshape(share * rows, cols)
        part = dot(grad, right)
        total = part if total is None else total + part
        back = dot(grad, left, TN)
        out_ref[pl.ds(first, share), 1, 0] = back.astype(BF).reshape(share, rows, cols)
    out_ref[:, 0, 0] = total.astype(BF).reshape(groups, rows, cols)


def triangle(sides, grads, axis=("z_lo", "core")):
    groups, _, per, rows, cols = sides.shape
    grad_spec = pl.BlockSpec((groups, 1, rows, cols), lambda c: (0, c, 0, 0))
    return call(
        lambda *refs: triangle_kernel(axis, *refs),
        pltpu.VMEM(sides.shape, BF),
        [kept(sides)] + [kept(g) for g in grads],
        [KEPT] + [grad_spec] * len(grads),
        pl.BlockSpec((groups, 2, 1, rows, cols), lambda c: (0, 0, c, 0, 0)),
        grid=(per,),
        flops=4 * 10**9,
        moved=5 * MIB,
    )


def gate_kernel(unroll, in_ref, factors_ref, normed_ref, w_ref, out_ref, raw_ref, flat, total):
    groups, _, per, rows, _ = in_ref.shape
    half = groups * per
    pairs = normed_ref.shape[0]
    step = pl.program_id(0)

    @pl.when(step == 0)
    def _():
        for g in range(groups):
            for side in range(2):
                for c in range(per):
                    first = (side * half + g * per + c) * rows
                    flat[first : first + rows, :] = in_ref[g, side, c].astype(F32)
        total[...] = jnp.zeros_like(total)

    w = w_ref[...].T

    def pair(q, carry):
        p = step * pairs + q
        parts = []
        for side in range(2):
            incoming = jnp.concatenate(
                [flat[pl.ds(side * half * rows + 2 * p + e, half, stride=rows), :] for e in range(2)], axis=1
            )
            at = 2 * side * half
            for first in (at, at + half):
                parts.append((incoming * factors_ref[q, first : first + half, :].astype(F32)).astype(BF))
        grads = jnp.concatenate(parts, axis=0)
        total[...] += dot(grads, normed_ref[q], NT)
        out_ref[q] = dot(w, grads).astype(BF)
        return carry

    lax.fori_loop(0, pairs, pair, 0, unroll=unroll)

    @pl.when(step == pl.num_programs(0) - 1)
    def _():
        raw_ref[...] = total[...].astype(BF)


def gate(incoming, factors, normed, w, unroll=8, step=8):
    groups, _, per, rows, cols = incoming.shape
    return call(
        lambda *refs: gate_kernel(unroll, *refs),
        [pltpu.VMEM(normed.shape, BF), pltpu.VMEM(w.shape, BF)],
        [kept(incoming), in_hbm(factors), in_hbm(normed), in_hbm(w)],
        [KEPT, leading(step, factors.shape), leading(step, normed.shape), fixed(w.shape)],
        [leading(step, normed.shape), fixed(w.shape)],
        [pltpu.VMEM((2 * groups * per * rows, cols), F32), pltpu.VMEM(w.shape, F32)],
        (normed.shape[0] // step,),
        flops=6 * 10**9,
        moved=8 * MIB,
    )


def finish_kernel(unit_ref, inv_ref, gain_ref, own_ref, other_ref, out_ref, gains):
    step, cols, depth = out_ref.shape

    @pl.when(pl.program_id(0) == 0)
    def _():
        gains[...] = jnp.broadcast_to(gain_ref[...], (2 * cols, depth)).T

    turn = identity(2 * cols).astype(BF)
    base = pl.program_id(0) * (step // 2)
    for q in range(step // 2):
        unit = unit_ref[q]
        scaled = (own_ref[base + q].astype(F32) + other_ref[base + q].astype(F32)) * gains[...]
        mean = jnp.mean(scaled, axis=0, keepdims=True)
        along = jnp.mean(scaled * unit, axis=0, keepdims=True)
        made = (inv_ref[q] * (scaled - mean - unit * along)).astype(BF)
        out_ref[pl.ds(2 * q, 2)] = dot(turn, made, NT).astype(BF).reshape(2, cols, depth)


def finish(unit, inv_std, gain, own, other, step=16):
    pairs, depth, twice = unit.shape
    shape = (2 * pairs, twice // 2, depth)
    half = step // 2
    return call(
        finish_kernel,
        jax.ShapeDtypeStruct(shape, BF),
        [in_hbm(unit), in_hbm(inv_std), in_hbm(gain[None]), kept(own), kept(other)],
        [leading(half, unit.shape), leading(half, inv_std.shape), fixed((1, depth)), KEPT, KEPT],
        leading(step, shape),
        [pltpu.VMEM((depth, twice), F32)],
        (shape[0] // step,),
        flops=10**9,
        moved=4 * MIB,
    )


def gather_kernel(pieces_ref, out_ref):
    count, _, _ = pieces_ref.shape
    total = pieces_ref[0]
    for n in range(1, count):
        total = total + pieces_ref[n]
    piece = total.astype(BF)
    for n in range(out_ref.shape[0]):
        out_ref[n] = piece


def summed_copies(pieces, count):
    out = pltpu.HBM((count,) + pieces.shape[1:], BF)
    return call(gather_kernel, out, [kept(pieces)], [KEPT], KEPT)


def clip_kernel(axis, pieces_ref, out_ref):
    count, rows, depth = pieces_ref.shape
    here = lax.axis_index(axis)
    total = jnp.zeros((rows, depth), F32)
    for n in range(count):
        piece = pieces_ref[n].astype(F32)
        total = total + piece * piece
    squares = jnp.sum(jnp.sum(total, axis=0, keepdims=True), axis=1, keepdims=True)
    factor = jnp.minimum(1.0, CLIP_LIMIT * lax.rsqrt(squares + 1e-06))
    for n in range(count // 2):
        out_ref[n * rows : (n + 1) * rows, :] = pieces_ref[2 * n + here].astype(F32) * factor


def clip(pieces, axis="col"):
    count, rows, depth = pieces.shape
    return call(
        lambda *refs: clip_kernel(axis, *refs),
        pltpu.HBM((count // 2 * rows, depth), F32),
        [kept(pieces)],
        [KEPT],
        KEPT,
    )


def swapped(x, axis):
    return lax.ppermute(x, axis, [(0, 1), (1, 0)])


def on_device(pair_rep, norm_gain, weights, residue_mask, product_grad):
    rows, cols, depth = pair_rep.shape
    chans = product_grad.shape[1]
    groups = lax.axis_size("ia")
    per = chans // groups
    w = jnp.swapaxes(weights, 1, 2).reshape(4 * chans, depth)

    grads = channels_first(product_grad).reshape(groups, per, rows, cols)
    grads = lax.all_to_all(grads, "ia", 0, 0, tiled=True)
    sides, factors, normed, unit, inv_std = project(pair_rep, norm_gain, w, residue_mask, groups)
    grads, sides = lax.optimization_barrier((grads, sides))
    far = swapped(grads, "z_lo")
    sides = lax.all_to_all(sides, "ia", 0, 0, tiled=True)
    near = swapped(grads, "core")
    farther = swapped(far, "core")
    products = triangle(sides, (grads, near, far, farther))
    products = lax.all_to_all(products, "ia", 0, 0, tiled=True)
    own, raw = gate(products, factors, normed, w)
    raw = raw.astype(F32) + swapped(raw, "z_lo").astype(F32)
    other = swapped(own, "col")
    peers = ("ia", "core")
    pieces = raw.reshape(lax.axis_size(peers), -1, depth)
    pieces = lax.all_to_all(pieces, peers, 0, 0, tiled=True)
    everyone = ("ia", "core", "col")
    copies = summed_copies(pieces, lax.axis_size(everyone))
    pieces = lax.all_to_all(copies, everyone, 0, 0, tiled=True)
    pair_grad = finish(unit, inv_std, norm_gain, own, other)
    pieces, pair_grad = lax.optimization_barrier((pieces, pair_grad))
    weight_grads = jnp.swapaxes(clip(pieces).reshape(4, chans, depth), 1, 2)
    return (pair_grad, weight_grads)


def solution(mesh):
    sizes = dict(mesh.shape)
    split = (sizes["ia"], sizes["ja"] // 2, 2, sizes["col"])
    fine = Mesh(mesh.devices.reshape(split), ("ia", "z_lo", "core", "col"))
    ja = ("z_lo", "core")
    return jax.shard_map(
        on_device,
        mesh=fine,
        in_specs=(P("ia", ja, None), P(), P(None, None, "col"), P(), P("ia", "col", ja)),
        out_specs=(P("ia", ja, None), P(None, None, "col")),
        check_vma=False,
    )
```

```python
import jax
import jax.numpy as jnp
from jax import lax
from jax.experimental import pallas as pl
from jax.experimental.pallas import tpu as pltpu
from jax.sharding import Mesh
from jax.sharding import PartitionSpec as P


CLIP_LIMIT = 64.0
BF, F32 = jnp.bfloat16, jnp.float32
NN = (((1,), (0,)), ((), ()))
NT = (((1,), (1,)), ((), ()))
TN = (((0,), (0,)), ((), ()))
KEPT = pl.BlockSpec(memory_space=pltpu.VMEM)
SCALARS = pl.BlockSpec(memory_space=pltpu.SMEM)
MIB = 2**20


def dot(a, b, dims=NN):
    return lax.dot_general(a, b, dims, preferred_element_type=F32)


def kept(x):
    return pltpu.with_memory_space_constraint(x, pltpu.VMEM)


def in_hbm(x):
    return pltpu.with_memory_space_constraint(x, pltpu.HBM)


def identity(size):
    row = lax.broadcasted_iota(jnp.int32, (size, size), 0)
    col = lax.broadcasted_iota(jnp.int32, (size, size), 1)
    return (row == col).astype(F32)


def call(kernel, out_shape, args, in_specs, out_specs, scratch=(), grid=(), flops=10**6, moved=MIB):
    return pl.pallas_call(
        kernel,
        grid=grid,
        out_shape=out_shape,
        in_specs=in_specs,
        out_specs=out_specs,
        scratch_shapes=list(scratch),
        compiler_params=pltpu.CompilerParams(vmem_limit_bytes=24 * MIB),
        cost_estimate=pl.CostEstimate(flops=flops, bytes_accessed=moved, transcendentals=0),
    )(*args)


def fixed(shape):
    return pl.BlockSpec(shape, lambda r: (0,) * len(shape))


def leading(step, shape):
    return pl.BlockSpec((step,) + tuple(shape[1:]), lambda r: (r,) + (0,) * (len(shape) - 1))


def channels_first_kernel(x_ref, out_ref, flat):
    rows, chans, width = x_ref.shape
    flat[...] = x_ref[...].reshape(rows * chans, width).astype(F32)
    for c in range(chans):
        out_ref[c] = flat[pl.ds(c, rows, stride=chans), :].astype(BF)


def channels_first(x, step=16):
    rows, chans, width = x.shape
    return call(
        channels_first_kernel,
        jax.ShapeDtypeStruct((chans, rows, width), BF),
        [x],
        [leading(step, x.shape)],
        pl.BlockSpec((chans, step, width), lambda r: (0, r, 0)),
        [pltpu.VMEM((step * chans, width), F32)],
        (rows // step,),
    )


def project_kernel(axes, unroll, x_ref, gain_ref, w_ref, mask_ref, cols_ref, sides_ref, factors_ref, normed_ref, unit_ref, inv_ref, flat, gains):
    rows, cols, depth = x_ref.shape
    groups, _, per, _, _ = sides_ref.shape
    half = groups * per
    step = pl.program_id(0)
    first_row = lax.axis_index(axes[0]) * (rows * pl.num_programs(0)) + step * rows
    centring = (identity(depth) - 1.0 / depth).astype(BF)

    @pl.when(step == 0)
    def _():
        gains[...] = jnp.broadcast_to(gain_ref[...], (2 * cols, depth)).T

    w = w_ref[...]
    valid_cols = cols_ref[pl.ds(lax.axis_index(axes[1]), 1), :].astype(F32)

    def pair(p, carry):
        x = x_ref[pl.ds(2 * p, 2)].reshape(2 * cols, depth)
        centred = dot(centring, x, NT)
        inv_std = lax.rsqrt(jnp.mean(centred * centred, axis=0, keepdims=True) + 1e-05)
        unit = centred * inv_std
        normed = (unit * gains[...]).astype(BF)
        unit_ref[p] = unit
        inv_ref[p] = inv_std
        normed_ref[p] = normed
        proj = dot(w, normed)
        valid = jnp.concatenate([valid_cols * mask_ref[first_row + 2 * p + e].astype(F32) for e in range(2)], axis=1)
        for side in range(2):
            at = 2 * side * half
            linear = proj[at : at + half]
            gate = jax.nn.sigmoid(proj[at + half : at + 2 * half])
            first = valid * gate
            both = first * linear
            for e in range(2):
                put = pl.multiple_of((2 * p + e) * 2 * half + side * half, half)
                flat[pl.ds(put, half), :] = both[:, e * cols : (e + 1) * cols]
            factors_ref[p, at : at + half, :] = first.astype(BF)
            factors_ref[p, at + half : at + 2 * half, :] = (both * (1.0 - gate)).astype(BF)
        return carry

    lax.fori_loop(0, rows // 2, pair, 0, unroll=unroll)
    for g in range(groups):
        for side in range(2):
            for c in range(per):
                first = side * half + g * per + c
                sides_ref[g, side, c] = flat[pl.ds(first, rows, stride=2 * half), :].astype(BF)


def project(x, gain, w, mask, groups, axes=("ia", ("z_lo", "core")), unroll=4, step=8):
    rows, cols, depth = x.shape
    half = w.shape[0] // 4
    per = half // groups
    pairs = rows // 2
    out = [
        pltpu.HBM((groups, 2, per, rows, cols), BF),
        pltpu.HBM((pairs, 4 * half, 2 * cols), BF),
        pltpu.HBM((pairs, depth, 2 * cols), BF),
        pltpu.HBM((pairs, depth, 2 * cols), F32),
        pltpu.HBM((pairs, 1, 2 * cols), F32),
    ]
    table = mask.reshape(-1, cols)
    return call(
        lambda *refs: project_kernel(axes, unroll, *refs),
        out,
        [in_hbm(x), in_hbm(gain[None]), in_hbm(w), mask, in_hbm(table)],
        [leading(step, x.shape), fixed((1, depth)), fixed(w.shape), SCALARS, fixed(table.shape)],
        [pl.BlockSpec((groups, 2, per, step, cols), lambda r: (0, 0, 0, r, 0))] + [leading(step // 2, o.shape) for o in out[1:]],
        [pltpu.VMEM((step * 2 * half, cols), F32), pltpu.VMEM((depth, 2 * cols), F32)],
        (rows // step,),
        flops=6 * 10**9,
        moved=8 * MIB,
    )


def triangle_kernel(axis, sides_ref, *refs):
    *grads, out_ref = refs
    groups, _, _, rows, cols = sides_ref.shape
    share = groups // len(grads)
    here = lax.axis_index(axis)
    c = pl.program_id(0)
    left = sides_ref[:, 0, c].reshape(groups * rows, cols)
    total = None
    for t, grad_ref in enumerate(grads):
        first = (here ^ t) * share
        grad = grad_ref[:, 0].reshape(groups * rows, cols)
        right = sides_ref[pl.ds(first, share), 1, c].reshape(share * rows, cols)
        part = dot(grad, right)
        total = part if total is None else total + part
        back = dot(grad, left, TN)
        out_ref[pl.ds(first, share), 1, 0] = back.astype(BF).reshape(share, rows, cols)
    out_ref[:, 0, 0] = total.astype(BF).reshape(groups, rows, cols)


def triangle(sides, grads, axis=("z_lo", "core")):
    groups, _, per, rows, cols = sides.shape
    grad_spec = pl.BlockSpec((groups, 1, rows, cols), lambda c: (0, c, 0, 0))
    return call(
        lambda *refs: triangle_kernel(axis, *refs),
        pltpu.VMEM(sides.shape, BF),
        [kept(sides)] + [kept(g) for g in grads],
        [KEPT] + [grad_spec] * len(grads),
        pl.BlockSpec((groups, 2, 1, rows, cols), lambda c: (0, 0, c, 0, 0)),
        grid=(per,),
        flops=4 * 10**9,
        moved=5 * MIB,
    )


def gate_kernel(unroll, in_ref, factors_ref, normed_ref, w_ref, out_ref, raw_ref, flat, total):
    groups, _, per, rows, _ = in_ref.shape
    half = groups * per
    pairs = normed_ref.shape[0]
    step = pl.program_id(0)

    @pl.when(step == 0)
    def _():
        for g in range(groups):
            for side in range(2):
                for c in range(per):
                    first = (side * half + g * per + c) * rows
                    flat[first : first + rows, :] = in_ref[g, side, c].astype(F32)
        total[...] = jnp.zeros_like(total)

    w = w_ref[...].T

    def pair(q, carry):
        p = step * pairs + q
        parts = []
        for side in range(2):
            incoming = jnp.concatenate(
                [flat[pl.ds(side * half * rows + 2 * p + e, half, stride=rows), :] for e in range(2)], axis=1
            )
            at = 2 * side * half
            for first in (at, at + half):
                parts.append((incoming * factors_ref[q, first : first + half, :].astype(F32)).astype(BF))
        grads = jnp.concatenate(parts, axis=0)
        total[...] += dot(grads, normed_ref[q], NT)
        out_ref[q] = dot(w, grads).astype(BF)
        return carry

    lax.fori_loop(0, pairs, pair, 0, unroll=unroll)

    @pl.when(step == pl.num_programs(0) - 1)
    def _():
        raw_ref[...] = total[...]


def gate(incoming, factors, normed, w, unroll=8, step=8):
    groups, _, per, rows, cols = incoming.shape
    return call(
        lambda *refs: gate_kernel(unroll, *refs),
        [pltpu.VMEM(normed.shape, BF), pltpu.VMEM(w.shape, F32)],
        [kept(incoming), in_hbm(factors), in_hbm(normed), in_hbm(w)],
        [KEPT, leading(step, factors.shape), leading(step, normed.shape), fixed(w.shape)],
        [leading(step, normed.shape), fixed(w.shape)],
        [pltpu.VMEM((2 * groups * per * rows, cols), F32), pltpu.VMEM(w.shape, F32)],
        (normed.shape[0] // step,),
        flops=6 * 10**9,
        moved=8 * MIB,
    )


def finish_kernel(unit_ref, inv_ref, gain_ref, own_ref, other_ref, out_ref, gains):
    step, cols, depth = out_ref.shape

    @pl.when(pl.program_id(0) == 0)
    def _():
        gains[...] = jnp.broadcast_to(gain_ref[...], (2 * cols, depth)).T

    turn = identity(2 * cols).astype(BF)
    base = pl.program_id(0) * (step // 2)
    for q in range(step // 2):
        unit = unit_ref[q]
        scaled = (own_ref[base + q].astype(F32) + other_ref[base + q].astype(F32)) * gains[...]
        mean = jnp.mean(scaled, axis=0, keepdims=True)
        along = jnp.mean(scaled * unit, axis=0, keepdims=True)
        made = (inv_ref[q] * (scaled - mean - unit * along)).astype(BF)
        out_ref[pl.ds(2 * q, 2)] = dot(turn, made, NT).astype(BF).reshape(2, cols, depth)


def finish(unit, inv_std, gain, own, other, step=16):
    pairs, depth, twice = unit.shape
    shape = (2 * pairs, twice // 2, depth)
    half = step // 2
    return call(
        finish_kernel,
        jax.ShapeDtypeStruct(shape, BF),
        [in_hbm(unit), in_hbm(inv_std), in_hbm(gain[None]), kept(own), kept(other)],
        [leading(half, unit.shape), leading(half, inv_std.shape), fixed((1, depth)), KEPT, KEPT],
        leading(step, shape),
        [pltpu.VMEM((depth, twice), F32)],
        (shape[0] // step,),
        flops=10**9,
        moved=4 * MIB,
    )


def gather_kernel(pieces_ref, out_ref):
    count, _, _ = pieces_ref.shape
    total = pieces_ref[0]
    for n in range(1, count):
        total = total + pieces_ref[n]
    piece = total.astype(BF)
    for n in range(out_ref.shape[0]):
        out_ref[n] = piece


def summed_copies(pieces, count):
    out = pltpu.HBM((count,) + pieces.shape[1:], BF)
    return call(gather_kernel, out, [kept(pieces)], [KEPT], KEPT)


def clip_kernel(axis, pieces_ref, out_ref):
    count, rows, depth = pieces_ref.shape
    here = lax.axis_index(axis)

    def whole(group, core, col):
        first = 8 * group + 2 * core + col
        return pieces_ref[first].astype(F32) + pieces_ref[first + 4].astype(F32)

    places = [(group, core) for group in range(count // 8) for core in range(2)]
    total = jnp.zeros((rows, depth), F32)
    for group, core in places:
        for col in range(2):
            piece = whole(group, core, col)
            total = total + piece * piece
    squares = jnp.sum(jnp.sum(total, axis=0, keepdims=True), axis=1, keepdims=True)
    factor = jnp.minimum(1.0, CLIP_LIMIT * lax.rsqrt(squares + 1e-06))
    for n, (group, core) in enumerate(places):
        out_ref[n * rows : (n + 1) * rows, :] = whole(group, core, here) * factor


def clip(pieces, axis="col"):
    count, rows, depth = pieces.shape
    return call(
        lambda *refs: clip_kernel(axis, *refs),
        pltpu.HBM((count // 4 * rows, depth), F32),
        [kept(pieces)],
        [KEPT],
        KEPT,
    )


def swapped(x, axis):
    return lax.ppermute(x, axis, [(0, 1), (1, 0)])


def on_device(pair_rep, norm_gain, weights, residue_mask, product_grad):
    rows, cols, depth = pair_rep.shape
    chans = product_grad.shape[1]
    groups = lax.axis_size("ia")
    per = chans // groups
    w = jnp.swapaxes(weights, 1, 2).reshape(4 * chans, depth)

    grads = channels_first(product_grad).reshape(groups, per, rows, cols)
    grads = lax.all_to_all(grads, "ia", 0, 0, tiled=True)
    sides, factors, normed, unit, inv_std = project(pair_rep, norm_gain, w, residue_mask, groups)
    grads, sides = lax.optimization_barrier((grads, sides))
    far = swapped(grads, "z_lo")
    sides = lax.all_to_all(sides, "ia", 0, 0, tiled=True)
    near = swapped(grads, "core")
    farther = swapped(far, "core")
    products = triangle(sides, (grads, near, far, farther))
    products = lax.all_to_all(products, "ia", 0, 0, tiled=True)
    own, raw = gate(products, factors, normed, w)
    other = swapped(own, "col")
    peers = ("ia", "core")
    pieces = raw.reshape(lax.axis_size(peers), -1, depth)
    pieces = lax.all_to_all(pieces, peers, 0, 0, tiled=True)
    everyone = ("ia", "z_lo", "core", "col")
    copies = summed_copies(pieces, lax.axis_size(everyone))
    pieces = lax.all_to_all(copies, everyone, 0, 0, tiled=True)
    pair_grad = finish(unit, inv_std, norm_gain, own, other)
    pieces, pair_grad = lax.optimization_barrier((pieces, pair_grad))
    weight_grads = jnp.swapaxes(clip(pieces).reshape(4, chans, depth), 1, 2)
    return (pair_grad, weight_grads)


def solution(mesh):
    sizes = dict(mesh.shape)
    split = (sizes["ia"], sizes["ja"] // 2, 2, sizes["col"])
    fine = Mesh(mesh.devices.reshape(split), ("ia", "z_lo", "core", "col"))
    ja = ("z_lo", "core")
    return jax.shard_map(
        on_device,
        mesh=fine,
        in_specs=(P("ia", ja, None), P(), P(None, None, "col"), P(), P("ia", "col", ja)),
        out_specs=(P("ia", ja, None), P(None, None, "col")),
        check_vma=False,
    )
```

```python
import jax
import jax.numpy as jnp
from jax import lax
from jax.experimental import pallas as pl
from jax.experimental.pallas import tpu as pltpu
from jax.sharding import Mesh
from jax.sharding import PartitionSpec as P


CLIP_LIMIT = 64.0
BF, F32 = jnp.bfloat16, jnp.float32
NN = (((1,), (0,)), ((), ()))
NT = (((1,), (1,)), ((), ()))
TN = (((0,), (0,)), ((), ()))
KEPT = pl.BlockSpec(memory_space=pltpu.VMEM)
SCALARS = pl.BlockSpec(memory_space=pltpu.SMEM)
MIB = 2**20


def dot(a, b, dims=NN):
    return lax.dot_general(a, b, dims, preferred_element_type=F32)


def kept(x):
    return pltpu.with_memory_space_constraint(x, pltpu.VMEM)


def in_hbm(x):
    return pltpu.with_memory_space_constraint(x, pltpu.HBM)


def identity(size):
    row = lax.broadcasted_iota(jnp.int32, (size, size), 0)
    col = lax.broadcasted_iota(jnp.int32, (size, size), 1)
    return (row == col).astype(F32)


def call(kernel, out_shape, args, in_specs, out_specs, scratch=(), grid=(), flops=10**6, moved=MIB):
    return pl.pallas_call(
        kernel,
        grid=grid,
        out_shape=out_shape,
        in_specs=in_specs,
        out_specs=out_specs,
        scratch_shapes=list(scratch),
        compiler_params=pltpu.CompilerParams(vmem_limit_bytes=24 * MIB),
        cost_estimate=pl.CostEstimate(flops=flops, bytes_accessed=moved, transcendentals=0),
    )(*args)


def fixed(shape):
    return pl.BlockSpec(shape, lambda r: (0,) * len(shape))


def leading(step, shape):
    return pl.BlockSpec((step,) + tuple(shape[1:]), lambda r: (r,) + (0,) * (len(shape) - 1))


def channels_first_kernel(x_ref, out_ref, flat):
    rows, chans, width = x_ref.shape
    flat[...] = x_ref[...].reshape(rows * chans, width).astype(F32)
    for c in range(chans):
        out_ref[c] = flat[pl.ds(c, rows, stride=chans), :].astype(BF)


def channels_first(x, step=16):
    rows, chans, width = x.shape
    return call(
        channels_first_kernel,
        jax.ShapeDtypeStruct((chans, rows, width), BF),
        [x],
        [leading(step, x.shape)],
        pl.BlockSpec((chans, step, width), lambda r: (0, r, 0)),
        [pltpu.VMEM((step * chans, width), F32)],
        (rows // step,),
    )


def project_kernel(axes, unroll, x_ref, gain_ref, w_ref, mask_ref, cols_ref, sides_ref, factors_ref, normed_ref, unit_ref, inv_ref, flat, gains):
    rows, cols, depth = x_ref.shape
    groups, _, per, _, _ = sides_ref.shape
    half = groups * per
    step = pl.program_id(0)
    first_row = lax.axis_index(axes[0]) * (rows * pl.num_programs(0)) + step * rows
    centring = (identity(depth) - 1.0 / depth).astype(BF)

    @pl.when(step == 0)
    def _():
        gains[...] = jnp.broadcast_to(gain_ref[...], (2 * cols, depth)).T

    w = w_ref[...]
    valid_cols = cols_ref[pl.ds(lax.axis_index(axes[1]), 1), :].astype(F32)

    def pair(p, carry):
        x = x_ref[pl.ds(2 * p, 2)].reshape(2 * cols, depth)
        centred = dot(centring, x, NT)
        inv_std = lax.rsqrt(jnp.mean(centred * centred, axis=0, keepdims=True) + 1e-05)
        unit = centred * inv_std
        normed = (unit * gains[...]).astype(BF)
        unit_ref[p] = unit.astype(BF)
        inv_ref[p] = inv_std
        normed_ref[p] = normed
        proj = dot(w, normed)
        valid = jnp.concatenate([valid_cols * mask_ref[first_row + 2 * p + e].astype(F32) for e in range(2)], axis=1)
        for side in range(2):
            at = 2 * side * half
            linear = proj[at : at + half]
            gate = jax.nn.sigmoid(proj[at + half : at + 2 * half])
            first = valid * gate
            both = first * linear
            for e in range(2):
                put = pl.multiple_of((2 * p + e) * 2 * half + side * half, half)
                flat[pl.ds(put, half), :] = both[:, e * cols : (e + 1) * cols]
            factors_ref[p, at : at + half, :] = first.astype(BF)
            factors_ref[p, at + half : at + 2 * half, :] = (both * (1.0 - gate)).astype(BF)
        return carry

    lax.fori_loop(0, rows // 2, pair, 0, unroll=unroll)
    for g in range(groups):
        for side in range(2):
            for c in range(per):
                first = side * half + g * per + c
                sides_ref[g, side, c] = flat[pl.ds(first, rows, stride=2 * half), :].astype(BF)


def project(x, gain, w, mask, groups, axes=("ia", ("z_lo", "core")), unroll=4, step=8):
    rows, cols, depth = x.shape
    half = w.shape[0] // 4
    per = half // groups
    pairs = rows // 2
    out = [
        pltpu.HBM((groups, 2, per, rows, cols), BF),
        pltpu.HBM((pairs, 4 * half, 2 * cols), BF),
        pltpu.HBM((pairs, depth, 2 * cols), BF),
        pltpu.HBM((pairs, depth, 2 * cols), BF),
        pltpu.HBM((pairs, 1, 2 * cols), F32),
    ]
    table = mask.reshape(-1, cols)
    return call(
        lambda *refs: project_kernel(axes, unroll, *refs),
        out,
        [in_hbm(x), in_hbm(gain[None]), in_hbm(w), mask, in_hbm(table)],
        [leading(step, x.shape), fixed((1, depth)), fixed(w.shape), SCALARS, fixed(table.shape)],
        [pl.BlockSpec((groups, 2, per, step, cols), lambda r: (0, 0, 0, r, 0))] + [leading(step // 2, o.shape) for o in out[1:]],
        [pltpu.VMEM((step * 2 * half, cols), F32), pltpu.VMEM((depth, 2 * cols), F32)],
        (rows // step,),
        flops=6 * 10**9,
        moved=8 * MIB,
    )


def triangle_kernel(axis, sides_ref, *refs):
    *grads, out_ref = refs
    groups, _, _, rows, cols = sides_ref.shape
    share = groups // len(grads)
    here = lax.axis_index(axis)
    c = pl.program_id(0)
    left = sides_ref[:, 0, c].reshape(groups * rows, cols)
    total = None
    for t, grad_ref in enumerate(grads):
        first = (here ^ t) * share
        grad = grad_ref[:, 0].reshape(groups * rows, cols)
        right = sides_ref[pl.ds(first, share), 1, c].reshape(share * rows, cols)
        part = dot(grad, right)
        total = part if total is None else total + part
        back = dot(grad, left, TN)
        out_ref[pl.ds(first, share), 1, 0] = back.astype(BF).reshape(share, rows, cols)
    out_ref[:, 0, 0] = total.astype(BF).reshape(groups, rows, cols)


def triangle(sides, grads, axis=("z_lo", "core")):
    groups, _, per, rows, cols = sides.shape
    grad_spec = pl.BlockSpec((groups, 1, rows, cols), lambda c: (0, c, 0, 0))
    return call(
        lambda *refs: triangle_kernel(axis, *refs),
        pltpu.VMEM(sides.shape, BF),
        [kept(sides)] + [kept(g) for g in grads],
        [KEPT] + [grad_spec] * len(grads),
        pl.BlockSpec((groups, 2, 1, rows, cols), lambda c: (0, 0, c, 0, 0)),
        grid=(per,),
        flops=4 * 10**9,
        moved=5 * MIB,
    )


def gate_kernel(unroll, in_ref, factors_ref, normed_ref, w_ref, out_ref, raw_ref, flat, total):
    groups, _, per, rows, _ = in_ref.shape
    half = groups * per
    pairs = normed_ref.shape[0]
    step = pl.program_id(0)

    @pl.when(step == 0)
    def _():
        for g in range(groups):
            for side in range(2):
                for c in range(per):
                    first = (side * half + g * per + c) * rows
                    flat[first : first + rows, :] = in_ref[g, side, c].astype(F32)
        total[...] = jnp.zeros_like(total)

    w = w_ref[...].T

    def pair(q, carry):
        p = step * pairs + q
        parts = []
        for side in range(2):
            incoming = jnp.concatenate(
                [flat[pl.ds(side * half * rows + 2 * p + e, half, stride=rows), :] for e in range(2)], axis=1
            )
            at = 2 * side * half
            for first in (at, at + half):
                parts.append((incoming * factors_ref[q, first : first + half, :].astype(F32)).astype(BF))
        grads = jnp.concatenate(parts, axis=0)
        total[...] += dot(grads, normed_ref[q], NT)
        out_ref[q] = dot(w, grads).astype(BF)
        return carry

    lax.fori_loop(0, pairs, pair, 0, unroll=unroll)

    @pl.when(step == pl.num_programs(0) - 1)
    def _():
        raw_ref[...] = total[...]


def gate(incoming, factors, normed, w, unroll=8, step=8):
    groups, _, per, rows, cols = incoming.shape
    return call(
        lambda *refs: gate_kernel(unroll, *refs),
        [pltpu.VMEM(normed.shape, BF), pltpu.VMEM(w.shape, F32)],
        [kept(incoming), in_hbm(factors), in_hbm(normed), in_hbm(w)],
        [KEPT, leading(step, factors.shape), leading(step, normed.shape), fixed(w.shape)],
        [leading(step, normed.shape), fixed(w.shape)],
        [pltpu.VMEM((2 * groups * per * rows, cols), F32), pltpu.VMEM(w.shape, F32)],
        (normed.shape[0] // step,),
        flops=6 * 10**9,
        moved=8 * MIB,
    )


def fetch_kernel(x_ref, out_ref):
    out_ref[...] = x_ref[...]


def fetch(x, step=8):
    spec = leading(step, x.shape)
    return call(fetch_kernel, pltpu.VMEM(x.shape, x.dtype), [in_hbm(x)], [spec], spec, grid=(x.shape[0] // step,), flops=10**9)


def finish_kernel(unit_ref, inv_ref, gain_ref, own_ref, other_ref, out_ref, gains):
    step, cols, depth = out_ref.shape

    @pl.when(pl.program_id(0) == 0)
    def _():
        gains[...] = jnp.broadcast_to(gain_ref[...], (2 * cols, depth)).T

    turn = identity(2 * cols).astype(BF)
    base = pl.program_id(0) * (step // 2)
    for q in range(step // 2):
        unit = unit_ref[q].astype(F32)
        scaled = (own_ref[base + q].astype(F32) + other_ref[base + q].astype(F32)) * gains[...]
        mean = jnp.mean(scaled, axis=0, keepdims=True)
        along = jnp.mean(scaled * unit, axis=0, keepdims=True)
        made = (inv_ref[q] * (scaled - mean - unit * along)).astype(BF)
        out_ref[pl.ds(2 * q, 2)] = dot(turn, made, NT).astype(BF).reshape(2, cols, depth)


def finish(unit, inv_std, gain, own, other, step=16):
    pairs, depth, twice = unit.shape
    shape = (2 * pairs, twice // 2, depth)
    half = step // 2
    return call(
        finish_kernel,
        jax.ShapeDtypeStruct(shape, BF),
        [kept(unit), in_hbm(inv_std), in_hbm(gain[None]), kept(own), kept(other)],
        [leading(half, unit.shape), leading(half, inv_std.shape), fixed((1, depth)), KEPT, KEPT],
        leading(step, shape),
        [pltpu.VMEM((depth, twice), F32)],
        (shape[0] // step,),
        flops=10**9,
        moved=4 * MIB,
    )


def gather_kernel(pieces_ref, out_ref):
    count, _, _ = pieces_ref.shape
    total = pieces_ref[0]
    for n in range(1, count):
        total = total + pieces_ref[n]
    piece = total.astype(BF)
    for n in range(out_ref.shape[0]):
        out_ref[n] = piece


def summed_copies(pieces, count):
    out = pltpu.HBM((count,) + pieces.shape[1:], BF)
    return call(gather_kernel, out, [kept(pieces)], [KEPT], KEPT)


def clip_kernel(axis, pieces_ref, out_ref):
    count, rows, depth = pieces_ref.shape
    here = lax.axis_index(axis)

    def whole(group, core, col):
        first = 8 * group + 2 * core + col
        return pieces_ref[first].astype(F32) + pieces_ref[first + 4].astype(F32)

    places = [(group, core) for group in range(count // 8) for core in range(2)]
    total = jnp.zeros((rows, depth), F32)
    for group, core in places:
        for col in range(2):
            piece = whole(group, core, col)
            total = total + piece * piece
    squares = jnp.sum(jnp.sum(total, axis=0, keepdims=True), axis=1, keepdims=True)
    factor = jnp.minimum(1.0, CLIP_LIMIT * lax.rsqrt(squares + 1e-06))
    for n, (group, core) in enumerate(places):
        out_ref[n * rows : (n + 1) * rows, :] = whole(group, core, here) * factor


def clip(pieces, axis="col"):
    count, rows, depth = pieces.shape
    return call(
        lambda *refs: clip_kernel(axis, *refs), pltpu.HBM((count // 4 * rows, depth), F32), [kept(pieces)], [KEPT], KEPT
    )


def swapped(x, axis):
    return lax.ppermute(x, axis, [(0, 1), (1, 0)])


def on_device(pair_rep, norm_gain, weights, residue_mask, product_grad):
    rows, cols, depth = pair_rep.shape
    chans = product_grad.shape[1]
    groups = lax.axis_size("ia")
    per = chans // groups
    w = jnp.swapaxes(weights, 1, 2).reshape(4 * chans, depth)

    grads = channels_first(product_grad).reshape(groups, per, rows, cols)
    grads = lax.all_to_all(grads, "ia", 0, 0, tiled=True)
    sides, factors, normed, unit, inv_std = project(pair_rep, norm_gain, w, residue_mask, groups)
    grads, sides = lax.optimization_barrier((grads, sides))
    far = swapped(grads, "z_lo")
    sides = lax.all_to_all(sides, "ia", 0, 0, tiled=True)
    near = swapped(grads, "core")
    farther = swapped(far, "core")
    products = triangle(sides, (grads, near, far, farther))
    products = lax.all_to_all(products, "ia", 0, 0, tiled=True)
    own, raw = gate(products, factors, normed, w)
    other = swapped(own, "col")
    peers = ("ia", "core")
    pieces = raw.reshape(lax.axis_size(peers), -1, depth)
    pieces = lax.all_to_all(pieces, peers, 0, 0, tiled=True)
    everyone = ("ia", "z_lo", "core", "col")
    copies = summed_copies(pieces, lax.axis_size(everyone))
    unit, copies = lax.optimization_barrier((unit, copies))
    pieces = lax.all_to_all(copies, everyone, 0, 0, tiled=True)
    unit = fetch(unit)
    pair_grad = finish(unit, inv_std, norm_gain, own, other)
    pieces, pair_grad = lax.optimization_barrier((pieces, pair_grad))
    weight_grads = jnp.swapaxes(clip(pieces).reshape(4, chans, depth), 1, 2)
    return (pair_grad, weight_grads)


def solution(mesh):
    sizes = dict(mesh.shape)
    split = (sizes["ia"], sizes["ja"] // 2, 2, sizes["col"])
    fine = Mesh(mesh.devices.reshape(split), ("ia", "z_lo", "core", "col"))
    ja = ("z_lo", "core")
    return jax.shard_map(
        on_device,
        mesh=fine,
        in_specs=(P("ia", ja, None), P(), P(None, None, "col"), P(), P("ia", "col", ja)),
        out_specs=(P("ia", ja, None), P(None, None, "col")),
        check_vma=False,
    )
```

```python
import jax
import jax.numpy as jnp
from jax import lax
from jax.experimental import pallas as pl
from jax.experimental.pallas import tpu as pltpu
from jax.sharding import Mesh
from jax.sharding import PartitionSpec as P


CLIP_LIMIT = 64.0
BF, F32 = jnp.bfloat16, jnp.float32
NN = (((1,), (0,)), ((), ()))
NT = (((1,), (1,)), ((), ()))
TN = (((0,), (0,)), ((), ()))
KEPT = pl.BlockSpec(memory_space=pltpu.VMEM)
SCALARS = pl.BlockSpec(memory_space=pltpu.SMEM)
MIB = 2**20


def dot(a, b, dims=NN):
    return lax.dot_general(a, b, dims, preferred_element_type=F32)


def kept(x):
    return pltpu.with_memory_space_constraint(x, pltpu.VMEM)


def in_hbm(x):
    return pltpu.with_memory_space_constraint(x, pltpu.HBM)


def identity(size):
    row = lax.broadcasted_iota(jnp.int32, (size, size), 0)
    col = lax.broadcasted_iota(jnp.int32, (size, size), 1)
    return (row == col).astype(F32)


def call(kernel, out_shape, args, in_specs, out_specs, scratch=(), grid=(), flops=10**6, moved=MIB):
    return pl.pallas_call(
        kernel,
        grid=grid,
        out_shape=out_shape,
        in_specs=in_specs,
        out_specs=out_specs,
        scratch_shapes=list(scratch),
        compiler_params=pltpu.CompilerParams(vmem_limit_bytes=24 * MIB),
        cost_estimate=pl.CostEstimate(flops=flops, bytes_accessed=moved, transcendentals=0),
    )(*args)


def fixed(shape):
    return pl.BlockSpec(shape, lambda r: (0,) * len(shape))


def leading(step, shape):
    return pl.BlockSpec((step,) + tuple(shape[1:]), lambda r: (r,) + (0,) * (len(shape) - 1))


def channels_first_kernel(x_ref, out_ref, flat):
    rows, chans, width = x_ref.shape
    flat[...] = x_ref[...].reshape(rows * chans, width).astype(F32)
    for c in range(chans):
        out_ref[c] = flat[pl.ds(c, rows, stride=chans), :].astype(BF)


def channels_first(x, step=16):
    rows, chans, width = x.shape
    return call(
        channels_first_kernel,
        jax.ShapeDtypeStruct((chans, rows, width), BF),
        [x],
        [leading(step, x.shape)],
        pl.BlockSpec((chans, step, width), lambda r: (0, r, 0)),
        [pltpu.VMEM((step * chans, width), F32)],
        (rows // step,),
    )


def project_kernel(axes, unroll, x_ref, gain_ref, w_ref, mask_ref, cols_ref, sides_ref, factors_ref, normed_ref, unit_ref, inv_ref, flat, gains):
    rows, cols, depth = x_ref.shape
    groups, _, per, _, _ = sides_ref.shape
    half = groups * per
    step = pl.program_id(0)
    first_row = lax.axis_index(axes[0]) * (rows * pl.num_programs(0)) + step * rows
    centring = (identity(depth) - 1.0 / depth).astype(BF)

    @pl.when(step == 0)
    def _():
        gains[...] = jnp.broadcast_to(gain_ref[...], (2 * cols, depth)).T

    w = w_ref[...]
    valid_cols = cols_ref[pl.ds(lax.axis_index(axes[1]), 1), :].astype(F32)

    def pair(p, carry):
        x = x_ref[pl.ds(2 * p, 2)].reshape(2 * cols, depth)
        centred = dot(centring, x, NT)
        inv_std = lax.rsqrt(jnp.mean(centred * centred, axis=0, keepdims=True) + 1e-05)
        unit = centred * inv_std
        normed = (unit * gains[...]).astype(BF)
        unit_ref[p] = unit.astype(BF)
        inv_ref[p] = inv_std
        normed_ref[p] = normed
        proj = dot(w, normed)
        valid = jnp.concatenate([valid_cols * mask_ref[first_row + 2 * p + e].astype(F32) for e in range(2)], axis=1)
        for side in range(2):
            at = 2 * side * half
            linear = proj[at : at + half]
            gate = jax.nn.sigmoid(proj[at + half : at + 2 * half])
            first = valid * gate
            both = first * linear
            for e in range(2):
                put = pl.multiple_of((2 * p + e) * 2 * half + side * half, half)
                flat[pl.ds(put, half), :] = both[:, e * cols : (e + 1) * cols]
            factors_ref[p, at : at + half, :] = first.astype(BF)
            factors_ref[p, at + half : at + 2 * half, :] = (both * (1.0 - gate)).astype(BF)
        return carry

    lax.fori_loop(0, rows // 2, pair, 0, unroll=unroll)
    for g in range(groups):
        for side in range(2):
            for c in range(per):
                first = side * half + g * per + c
                sides_ref[g, side, c] = flat[pl.ds(first, rows, stride=2 * half), :].astype(BF)


def project(x, gain, w, mask, groups, axes=("ia", ("z_lo", "core")), unroll=4, step=8):
    rows, cols, depth = x.shape
    half = w.shape[0] // 4
    per = half // groups
    pairs = rows // 2
    out = [
        pltpu.HBM((groups, 2, per, rows, cols), BF),
        pltpu.HBM((pairs, 4 * half, 2 * cols), BF),
        pltpu.HBM((pairs, depth, 2 * cols), BF),
        pltpu.HBM((pairs, depth, 2 * cols), BF),
        pltpu.HBM((pairs, 1, 2 * cols), F32),
    ]
    table = mask.reshape(-1, cols)
    return call(
        lambda *refs: project_kernel(axes, unroll, *refs),
        out,
        [in_hbm(x), in_hbm(gain[None]), in_hbm(w), mask, in_hbm(table)],
        [leading(step, x.shape), fixed((1, depth)), fixed(w.shape), SCALARS, fixed(table.shape)],
        [pl.BlockSpec((groups, 2, per, step, cols), lambda r: (0, 0, 0, r, 0))] + [leading(step // 2, o.shape) for o in out[1:]],
        [pltpu.VMEM((step * 2 * half, cols), F32), pltpu.VMEM((depth, 2 * cols), F32)],
        (rows // step,),
        flops=6 * 10**9,
        moved=8 * MIB,
    )


def triangle_kernel(axis, sides_ref, *refs):
    *grads, out_ref = refs
    groups, _, _, rows, cols = sides_ref.shape
    share = groups // len(grads)
    here = lax.axis_index(axis)
    c = pl.program_id(0)
    left = sides_ref[:, 0, c].reshape(groups * rows, cols)
    total = None
    for t, grad_ref in enumerate(grads):
        first = (here ^ t) * share
        grad = grad_ref[:, 0].reshape(groups * rows, cols)
        right = sides_ref[pl.ds(first, share), 1, c].reshape(share * rows, cols)
        part = dot(grad, right)
        total = part if total is None else total + part
        back = dot(grad, left, TN)
        out_ref[pl.ds(first, share), 1, 0] = back.astype(BF).reshape(share, rows, cols)
    out_ref[:, 0, 0] = total.astype(BF).reshape(groups, rows, cols)


def triangle(sides, grads, axis=("z_lo", "core")):
    groups, _, per, rows, cols = sides.shape
    grad_spec = pl.BlockSpec((groups, 1, rows, cols), lambda c: (0, c, 0, 0))
    return call(
        lambda *refs: triangle_kernel(axis, *refs),
        pltpu.VMEM(sides.shape, BF),
        [kept(sides)] + [kept(g) for g in grads],
        [KEPT] + [grad_spec] * len(grads),
        pl.BlockSpec((groups, 2, 1, rows, cols), lambda c: (0, 0, c, 0, 0)),
        grid=(per,),
        flops=4 * 10**9,
        moved=5 * MIB,
    )


def gate_kernel(unroll, in_ref, factors_ref, normed_ref, w_ref, out_ref, raw_ref, flat, total):
    groups, _, per, rows, _ = in_ref.shape
    half = groups * per
    pairs = normed_ref.shape[0]
    step = pl.program_id(0)

    @pl.when(step == 0)
    def _():
        for g in range(groups):
            for side in range(2):
                for c in range(per):
                    first = (side * half + g * per + c) * rows
                    flat[first : first + rows, :] = in_ref[g, side, c].astype(F32)
        total[...] = jnp.zeros_like(total)

    w = w_ref[...].T

    def pair(q, carry):
        p = step * pairs + q
        parts = []
        for side in range(2):
            incoming = jnp.concatenate(
                [flat[pl.ds(side * half * rows + 2 * p + e, half, stride=rows), :] for e in range(2)], axis=1
            )
            at = 2 * side * half
            for first in (at, at + half):
                parts.append((incoming * factors_ref[q, first : first + half, :].astype(F32)).astype(BF))
        grads = jnp.concatenate(parts, axis=0)
        total[...] += dot(grads, normed_ref[q], NT)
        out_ref[q] = dot(w, grads).astype(BF)
        return carry

    lax.fori_loop(0, pairs, pair, 0, unroll=unroll)

    @pl.when(step == pl.num_programs(0) - 1)
    def _():
        raw_ref[...] = total[...].astype(BF)


def gate(incoming, factors, normed, w, unroll=8, step=8):
    groups, _, per, rows, cols = incoming.shape
    return call(
        lambda *refs: gate_kernel(unroll, *refs),
        [pltpu.VMEM(normed.shape, BF), pltpu.VMEM(w.shape, BF)],
        [kept(incoming), in_hbm(factors), in_hbm(normed), in_hbm(w)],
        [KEPT, leading(step, factors.shape), leading(step, normed.shape), fixed(w.shape)],
        [leading(step, normed.shape), fixed(w.shape)],
        [pltpu.VMEM((2 * groups * per * rows, cols), F32), pltpu.VMEM(w.shape, F32)],
        (normed.shape[0] // step,),
        flops=6 * 10**9,
        moved=8 * MIB,
    )


def fetch_kernel(x_ref, out_ref):
    out_ref[...] = x_ref[...]


def fetch(x, step=8):
    spec = leading(step, x.shape)
    return call(fetch_kernel, pltpu.VMEM(x.shape, x.dtype), [in_hbm(x)], [spec], spec, grid=(x.shape[0] // step,), flops=10**9)


def finish_kernel(unit_ref, inv_ref, gain_ref, own_ref, other_ref, out_ref, gains):
    step, cols, depth = out_ref.shape

    @pl.when(pl.program_id(0) == 0)
    def _():
        gains[...] = jnp.broadcast_to(gain_ref[...], (2 * cols, depth)).T

    turn = identity(2 * cols).astype(BF)
    base = pl.program_id(0) * (step // 2)
    for q in range(step // 2):
        unit = unit_ref[q].astype(F32)
        scaled = (own_ref[base + q].astype(F32) + other_ref[base + q].astype(F32)) * gains[...]
        mean = jnp.mean(scaled, axis=0, keepdims=True)
        along = jnp.mean(scaled * unit, axis=0, keepdims=True)
        made = (inv_ref[q] * (scaled - mean - unit * along)).astype(BF)
        out_ref[pl.ds(2 * q, 2)] = dot(turn, made, NT).astype(BF).reshape(2, cols, depth)


def finish(unit, inv_std, gain, own, other, step=16):
    pairs, depth, twice = unit.shape
    shape = (2 * pairs, twice // 2, depth)
    half = step // 2
    return call(
        finish_kernel,
        jax.ShapeDtypeStruct(shape, BF),
        [kept(unit), in_hbm(inv_std), in_hbm(gain[None]), kept(own), kept(other)],
        [leading(half, unit.shape), leading(half, inv_std.shape), fixed((1, depth)), KEPT, KEPT],
        leading(step, shape),
        [pltpu.VMEM((depth, twice), F32)],
        (shape[0] // step,),
        flops=10**9,
        moved=4 * MIB,
    )


def gather_kernel(pieces_ref, out_ref):
    count, _, _ = pieces_ref.shape
    total = pieces_ref[0].astype(F32)
    for n in range(1, count):
        total = total + pieces_ref[n].astype(F32)
    piece = total.astype(BF)
    for n in range(out_ref.shape[0]):
        out_ref[n] = piece


def summed_copies(pieces, count):
    out = pltpu.HBM((count,) + pieces.shape[1:], BF)
    return call(gather_kernel, out, [kept(pieces)], [KEPT], KEPT)


def clip_kernel(axis, pieces_ref, out_ref):
    count, rows, depth = pieces_ref.shape
    here = lax.axis_index(axis)

    def whole(group, core, col):
        first = 8 * group + 2 * core + col
        return pieces_ref[first].astype(F32) + pieces_ref[first + 4].astype(F32)

    places = [(group, core) for group in range(count // 8) for core in range(2)]
    total = jnp.zeros((rows, depth), F32)
    for group, core in places:
        for col in range(2):
            piece = whole(group, core, col)
            total = total + piece * piece
    squares = jnp.sum(jnp.sum(total, axis=0, keepdims=True), axis=1, keepdims=True)
    factor = jnp.minimum(1.0, CLIP_LIMIT * lax.rsqrt(squares + 1e-06))
    for n, (group, core) in enumerate(places):
        out_ref[n * rows : (n + 1) * rows, :] = whole(group, core, here) * factor


def clip(pieces, axis="col"):
    count, rows, depth = pieces.shape
    return call(
        lambda *refs: clip_kernel(axis, *refs), pltpu.HBM((count // 4 * rows, depth), F32), [kept(pieces)], [KEPT], KEPT
    )


def swapped(x, axis):
    return lax.ppermute(x, axis, [(0, 1), (1, 0)])


def on_device(pair_rep, norm_gain, weights, residue_mask, product_grad):
    rows, cols, depth = pair_rep.shape
    chans = product_grad.shape[1]
    groups = lax.axis_size("ia")
    per = chans // groups
    w = jnp.swapaxes(weights, 1, 2).reshape(4 * chans, depth)

    grads = channels_first(product_grad).reshape(groups, per, rows, cols)
    grads = lax.all_to_all(grads, "ia", 0, 0, tiled=True)
    sides, factors, normed, unit, inv_std = project(pair_rep, norm_gain, w, residue_mask, groups)
    grads, sides = lax.optimization_barrier((grads, sides))
    far = swapped(grads, "z_lo")
    sides = lax.all_to_all(sides, "ia", 0, 0, tiled=True)
    near = swapped(grads, "core")
    farther = swapped(far, "core")
    products = triangle(sides, (grads, near, far, farther))
    products = lax.all_to_all(products, "ia", 0, 0, tiled=True)
    own, raw = gate(products, factors, normed, w)
    other = swapped(own, "col")
    peers = ("ia", "core")
    pieces = raw.reshape(lax.axis_size(peers), -1, depth)
    pieces = lax.all_to_all(pieces, peers, 0, 0, tiled=True)
    everyone = ("ia", "z_lo", "core", "col")
    copies = summed_copies(pieces, lax.axis_size(everyone))
    unit, copies = lax.optimization_barrier((unit, copies))
    pieces = lax.all_to_all(copies, everyone, 0, 0, tiled=True)
    unit = fetch(unit)
    pair_grad = finish(unit, inv_std, norm_gain, own, other)
    pieces, pair_grad = lax.optimization_barrier((pieces, pair_grad))
    weight_grads = jnp.swapaxes(clip(pieces).reshape(4, chans, depth), 1, 2)
    return (pair_grad, weight_grads)


def solution(mesh):
    sizes = dict(mesh.shape)
    split = (sizes["ia"], sizes["ja"] // 2, 2, sizes["col"])
    fine = Mesh(mesh.devices.reshape(split), ("ia", "z_lo", "core", "col"))
    ja = ("z_lo", "core")
    return jax.shard_map(
        on_device,
        mesh=fine,
        in_specs=(P("ia", ja, None), P(), P(None, None, "col"), P(), P("ia", "col", ja)),
        out_specs=(P("ia", ja, None), P(None, None, "col")),
        check_vma=False,
    )
```
